32 devices in a mesh: row: 4 (over y, core), col: 8 (over z, x).
Axes of the slice: x: 2, y: 2, z: 4, core: 2. Of those that a mesh axis runs over, the one named last changes fastest.
Arguments:
- x_blocks: bfloat16 [4, 8, 21, 128, 128], P('row', 'col'), may hold values from -1.1953125 to 1.1953125
- x_slots: int32 [4, 8, 21], replicated, may hold values from 0 to 127, as said below
- x_count: int32 [4, 8], replicated, may hold values from 10 to 21, as said below
- s_slots: int32 [4, 8, 2], replicated, may hold values from 0 to 15, as said below
- s_count: int32 [4, 8], replicated, may hold values from 1 to 2, as said below
Outputs:
- square_blocks: bfloat16 [4, 8, 2, 128, 128], P('row', 'col')
- result_blocks: bfloat16 [4, 8, 2, 128, 128], P('row', 'col')
The draws below stay inside these ranges and needn't reach their ends.
Inputs may be any that keep to these rules, and one draw needn't show every extreme that they name: `x_slots`: in each tile the live slots hold distinct positions; the live blocks whose position % 16 is below 2 come first among the live slots, at most 2 of them, and some tile has exactly 2. Positions of slots that are not live are arbitrary within the range. `x_count`: some tile has exactly 21 live slots. `s_slots`: in each tile the live slots hold distinct positions. `s_count`: some tile has exactly 2 live slots.
All inputs are finite; a program needn't handle non-finite values.
Results may differ from the reference program's by a relative error of at most 0.0049.
Values may be sent and summed in bfloat16 or wider, within the bound.
No kernel may reach another device: no remote copies, remote signals or barrier semaphores. Data moves between devices by JAX's collectives and lax.ppermute only.
A program may use at most 128 MiB of HBM per device.

```python
import jax
import jax.numpy as jnp
from jax import lax

BLOCK = 128
RB = 8
JW = 2
NB = 64
KB = 16
CAPW = 2
CAPX = 21
CAPS = 2
N_ROW = 4
N_COL = 8


def tile_layout(key):
    tile_total = N_ROW * N_COL
    base_key = jax.random.fold_in(key, 41)
    keys_all = jax.random.split(base_key, 7)
    lowest = CAPX // 2
    x_total = jax.random.randint(keys_all[0], (tile_total,), lowest, CAPX + 1)
    window_total = jax.random.randint(keys_all[1], (tile_total,), 0, CAPW + 1)
    chosen = jax.random.randint(keys_all[2], (2,), 0, tile_total)
    x_total = x_total.at[chosen[0]].set(CAPX)
    window_total = window_total.at[chosen[1]].set(CAPW)
    window_total = jnp.minimum(window_total, x_total)
    window_cells = RB * JW
    other_cells = RB * (KB - JW)
    near_range = jnp.arange(window_cells, dtype=jnp.int32)
    far_range = jnp.arange(other_cells, dtype=jnp.int32)
    near_pos = near_range // JW * KB + near_range % JW
    far_pos = far_range // (KB - JW) * KB + JW + far_range % (KB - JW)
    tile_keys = jax.random.split(keys_all[3], tile_total)

    def one_tile(tile_key, win_count, all_count):
        first_key, second_key = jax.random.split(tile_key)
        near_order = jax.random.permutation(first_key, window_cells)
        far_order = jax.random.permutation(second_key, other_cells)
        candidates = jnp.concatenate([near_pos[near_order], far_pos[far_order]])
        rank_keys = jnp.concatenate([jnp.where(near_range < win_count, 0, 2), jnp.where(far_range < all_count - win_count, 1, 2)])
        arranged = jnp.argsort(rank_keys, stable=True)
        return candidates[arranged][:CAPX].astype(jnp.int32)
    x_slots = jax.vmap(one_tile)(tile_keys, window_total, x_total)
    s_total = jax.random.randint(keys_all[4], (tile_total,), 1, CAPS + 1)
    s_total = s_total.at[jax.random.randint(keys_all[5], (), 0, tile_total)].set(CAPS)
    s_keys = jax.random.split(keys_all[6], tile_total)

    def one_mask(mask_key):
        return jax.random.permutation(mask_key, window_cells)[:CAPS].astype(jnp.int32)
    s_slots = jax.vmap(one_mask)(s_keys)
    return (x_slots.reshape(N_ROW, N_COL, CAPX), x_total.astype(jnp.int32).reshape(N_ROW, N_COL), s_slots.reshape(N_ROW, N_COL, CAPS), s_total.astype(jnp.int32).reshape(N_ROW, N_COL))


def draw_x_slots(key, part):
    return tile_layout(key)[0]


def draw_x_count(key, part):
    return tile_layout(key)[1]


def draw_s_slots(key, part):
    return tile_layout(key)[2]


def draw_s_count(key, part):
    return tile_layout(key)[3]


def block_levels(stream_key, dims, pieces, smallest, top_value):
    factor_of = 1.0
    for dim, blocks in pieces:
        draws = jax.random.uniform(jax.random.fold_in(jax.random.fold_in(stream_key, 6), dim), (blocks,), jnp.float32, smallest / len(pieces), top_value / len(pieces))
        factor_of = factor_of * jnp.repeat(jnp.exp(draws), dims[dim] // blocks).reshape((-1,) + (1,) * (len(dims) - 1 - dim))
    return factor_of


def noise(own_key, dims, deviation, reach, pieces=(), held_as=jnp.bfloat16):
    array = deviation * jax.random.normal(own_key, dims, jnp.float32)
    if pieces:
        array = array * block_levels(own_key, dims, pieces, -0.22, 0.18)
    return jnp.clip(array, -reach, reach).astype(held_as)


def setup_inputs(seed: int = 0) -> dict:
    key_list = jax.random.split(jax.random.key(seed), 6)
    x_blocks = noise(key_list[0], (N_ROW, N_COL, CAPX, BLOCK, BLOCK), 0.2, 1.1953125, ((0, 4), (1, 8)))
    x_slots = draw_x_slots(jax.random.fold_in(key_list[5], 71), 0)
    x_count = draw_x_count(jax.random.fold_in(key_list[5], 71), 0)
    s_slots = draw_s_slots(jax.random.fold_in(key_list[5], 71), 0)
    s_count = draw_s_count(jax.random.fold_in(key_list[5], 71), 0)
    return dict(x_blocks=x_blocks, x_slots=x_slots, x_count=x_count, s_slots=s_slots, s_count=s_count)


def place_sum(left_part, right_part, inner_col):
    products = jnp.einsum("nrxy,nyz->nrxz", left_part.astype(jnp.float32), right_part.astype(jnp.float32), precision=lax.Precision.HIGHEST)
    placing = (inner_col[:, None] == jnp.arange(JW, dtype=jnp.int32)[None, :]).astype(jnp.float32)
    return jnp.einsum("nj,nrxz->rjxz", placing, products, precision=lax.Precision.HIGHEST)


def reference(x_blocks, x_slots, x_count, s_slots, s_count):
    sentinel = N_ROW * N_COL * CAPX
    stacked = x_blocks.reshape(sentinel, BLOCK, BLOCK)
    padded = jnp.concatenate([stacked, jnp.zeros((1, BLOCK, BLOCK), stacked.dtype)], axis=0)
    ordinal = jnp.arange(CAPX, dtype=jnp.int32)
    slot_live = ordinal[None, None, :] < x_count[:, :, None]
    grid_row = jnp.arange(N_COL, dtype=jnp.int32)[None, :, None] * RB + x_slots // KB
    grid_col = jnp.arange(N_ROW, dtype=jnp.int32)[:, None, None] * KB + x_slots % KB
    grid_row = jnp.where(slot_live, grid_row, NB).astype(jnp.int32)
    grid_col = jnp.where(slot_live, grid_col, NB).astype(jnp.int32)
    slot_ids = jnp.arange(sentinel, dtype=jnp.int32).reshape(N_ROW, N_COL, CAPX)
    slot_table = jnp.full((NB + 1, NB + 1), sentinel, jnp.int32).at[grid_row, grid_col].set(slot_ids)
    col_ids = jnp.arange(N_COL, dtype=jnp.int32)[:, None]

    def multiply(col_id, right_vals, inner_row, inner_col, usable):
        row_lanes = col_id * RB + jnp.arange(RB, dtype=jnp.int32)
        picked = slot_table[row_lanes[None, :], inner_row[:, None]]
        left_part = padded[picked]
        right_part = jnp.where(usable[:, None, None], right_vals, jnp.zeros_like(right_vals))
        return place_sum(left_part, right_part, inner_col)

    def first_tile(tile_index):
        row_id = tile_index // N_COL
        col_id = tile_index % N_COL
        positions = x_slots[row_id][:, :CAPW]
        counts = x_count[row_id]
        inner_row = (col_ids * RB + positions // KB).reshape(-1)
        inner_col = (positions % KB).reshape(-1)
        usable = ((jnp.arange(CAPW, dtype=jnp.int32)[None, :] < counts[:, None]) & (positions % KB < JW)).reshape(-1)
        right_vals = x_blocks[row_id][:, :CAPW].reshape(N_COL * CAPW, BLOCK, BLOCK)
        product = multiply(col_id, right_vals, inner_row, inner_col, usable)
        own_slots = s_slots[row_id, col_id]
        own_live = jnp.arange(CAPS, dtype=jnp.int32) < s_count[row_id, col_id]
        chosen = product.reshape(RB * JW, BLOCK, BLOCK)[own_slots]
        return jnp.where(own_live[:, None, None], chosen, 0.0).astype(jnp.bfloat16)

    squares = lax.map(first_tile, jnp.arange(N_ROW * N_COL, dtype=jnp.int32))
    squares = squares.reshape(N_ROW, N_COL, CAPS, BLOCK, BLOCK)

    def second_tile(tile_index):
        row_id = tile_index // N_COL
        col_id = tile_index % N_COL
        positions = s_slots[row_id]
        counts = s_count[row_id]
        inner_row = (col_ids * RB + positions // JW).reshape(-1)
        inner_col = (positions % JW).reshape(-1)
        usable = (jnp.arange(CAPS, dtype=jnp.int32)[None, :] < counts[:, None]).reshape(-1)
        right_vals = squares[row_id].reshape(N_COL * CAPS, BLOCK, BLOCK)
        product = multiply(col_id, right_vals, inner_row, inner_col, usable)
        own_slots = s_slots[row_id, col_id]
        own_live = jnp.arange(CAPS, dtype=jnp.int32) < s_count[row_id, col_id]
        own_block = padded[slot_table[col_id * RB + own_slots // JW, row_id * KB + own_slots % JW]].astype(jnp.float32)
        combined = 1.5 * own_block - 0.5 * product.reshape(RB * JW, BLOCK, BLOCK)[own_slots]
        return jnp.where(own_live[:, None, None], combined, 0.0).astype(jnp.bfloat16)

    results = lax.map(second_tile, jnp.arange(N_ROW * N_COL, dtype=jnp.int32))
    results = results.reshape(N_ROW, N_COL, CAPS, BLOCK, BLOCK)
    return squares, results
```

```python
import jax
import jax.numpy as jnp
from jax import lax
from jax.experimental import pallas as pl
from jax.experimental.pallas import tpu as pltpu
from jax.sharding import PartitionSpec as P

RB = 8
JW = 2
CAPW = 2


def pow2(n):
    return n & (n - 1) == 0


def partner(i, k, n):
    return i ^ k if pow2(n) else (i + k) % n


def origin(i, k, n):
    return jnp.bitwise_xor(i, k) if pow2(n) else lax.rem(i + (n - k), n)


def permute(x, axis, k, n):
    return lax.ppermute(x, axis, [(i, partner(i, k, n)) for i in range(n)])


def gather_col(x, n):
    parts = [x] + [None] * (n - 1)
    if n >= 4 and pow2(n):
        half = n // 2
        far = permute(x, "col", half, n)
        parts[half] = far
        for k in range(1, half):
            parts[k] = permute(x, "col", k, n)
        for k in range(1, half):
            parts[half + k] = permute(far, "col", k, n)
    else:
        for k in range(1, n):
            parts[k] = permute(x, "col", k, n)
    return parts


def match_index(targets, slot_keys, slot_live):
    matches = (targets[..., None] == slot_keys) & slot_live
    ordinal = jnp.arange(1, slot_keys.shape[0] + 1, dtype=jnp.int32)
    located = jnp.sum(jnp.where(matches, ordinal, 0), axis=-1)
    return jnp.where(located > 0, located - 1, slot_keys.shape[0])


def ordered(parts, me, n):
    stacked = jnp.stack(parts)
    ids = jnp.stack([origin(me, k, n) for k in range(n)])
    order = jnp.argsort(ids)
    return jnp.take(stacked, order, axis=0)


def general(x_blocks, x_slots, x_count, s_slots, s_count):
    nr, nc = lax.axis_size("row"), lax.axis_size("col")
    row_id, col_id = lax.axis_index("row"), lax.axis_index("col")
    capacity, size = x_blocks.shape[2], x_blocks.shape[3]
    order_blocks = RB * nc
    tile_width = order_blocks // nr
    tile = x_blocks[0, 0]
    panel = ordered([tile] + [permute(tile, "row", k, nr) for k in range(1, nr)], row_id, nr)
    stacked = panel.reshape(nr * capacity, size, size)
    padded = jnp.concatenate([stacked, jnp.zeros((1, size, size), stacked.dtype)], axis=0)
    column_slots = x_slots[:, col_id]
    column_count = x_count[:, col_id]
    ordinal = jnp.arange(capacity, dtype=jnp.int32)
    panel_live = (ordinal[None, :] < column_count[:, None]).reshape(-1)
    owners = jnp.arange(nr, dtype=jnp.int32)[:, None]
    panel_keys = (
        column_slots // tile_width * order_blocks + owners * tile_width + column_slots % tile_width
    ).reshape(-1)
    lanes = jnp.arange(RB, dtype=jnp.int32)

    def multiply(values, inner_row, inner_col, usable):
        picked = match_index(
            lanes[None, :] * order_blocks + inner_row[:, None], panel_keys, panel_live
        )

        def one(n, total):
            left = jnp.take(padded, picked[n], axis=0)
            right = jnp.where(usable[n], values[n], jnp.zeros_like(values[n]))
            part = jnp.einsum("rxy,yz->rxz", left, right, preferred_element_type=jnp.float32)
            column = jnp.clip(inner_col[n], 0, JW - 1)
            return total.at[:, column].add(part)

        start = jnp.zeros((RB, JW, size, size), jnp.float32)
        return lax.fori_loop(0, values.shape[0], one, start).reshape(RB * JW, size, size)

    def spread(table, counts, slots, stride):
        owner_ids = jnp.arange(nc, dtype=jnp.int32)[:, None]
        positions = table[:, :slots]
        inner_row = owner_ids * RB + positions // stride
        inner_col = positions % stride
        usable = (jnp.arange(slots, dtype=jnp.int32)[None, :] < counts[:, None]) & (inner_col < JW)
        return inner_row.reshape(-1), inner_col.reshape(-1), usable.reshape(-1)

    def columns(mine):
        parts = [mine] + [permute(mine, "col", k, nc) for k in range(1, nc)]
        return ordered(parts, col_id, nc).reshape(-1, size, size)

    first = multiply(
        columns(tile[:CAPW]), *spread(x_slots[row_id], x_count[row_id], CAPW, tile_width)
    )
    own_slots = s_slots[row_id, col_id]
    own_live = jnp.arange(own_slots.shape[0], dtype=jnp.int32) < s_count[row_id, col_id]
    square = jnp.where(
        own_live[:, None, None], jnp.take(first, own_slots, axis=0), 0.0
    ).astype(jnp.bfloat16)
    second = multiply(
        columns(square), *spread(s_slots[row_id], s_count[row_id], own_slots.shape[0], JW)
    )
    own_keys = own_slots // JW * order_blocks + row_id * tile_width + own_slots % JW
    own_block = jnp.take(padded, match_index(own_keys, panel_keys, panel_live), axis=0)
    combined = 1.5 * own_block.astype(jnp.float32) - 0.5 * jnp.take(second, own_slots, axis=0)
    result = jnp.where(own_live[:, None, None], combined, 0.0).astype(jnp.bfloat16)
    return square, result


def longest_list(x_slots, x_count, s_slots, s_count, tile_width):
    nr, nc, capacity = x_slots.shape
    caps = s_slots.shape[2]
    group = tile_width // RB
    live_x = jnp.arange(capacity, dtype=jnp.int32) < x_count[..., None]
    live_s = jnp.arange(caps, dtype=jnp.int32) < s_count[..., None]
    base = (jnp.arange(nc, dtype=jnp.int32) % group * RB)[None, :, None]
    near = x_slots[..., :CAPW]
    inner = jnp.concatenate([base + near // tile_width, base + s_slots // JW], axis=-1)
    column = jnp.concatenate([near % tile_width, s_slots % JW], axis=-1)
    live = jnp.concatenate([live_x[..., :CAPW], live_s], axis=-1)
    inner = inner.reshape(nr, 1, 1, nr, group * (CAPW + caps))
    column = jnp.where(live, column, -1).reshape(nr, 1, 1, nr, group * (CAPW + caps))
    out_row = (s_slots // JW * tile_width)[..., None, None]
    out_col = jnp.where(live_s, s_slots % JW, -2)[..., None, None]
    wanted = jnp.where(out_col == column, out_row + inner, -1)
    held = jnp.where(live_x, x_slots, -2).transpose(1, 0, 2)
    found = wanted[..., None] == held[None, :, None, :, None, :]
    return jnp.max(jnp.sum(found.astype(jnp.int32), axis=(2, 4, 5)))


def lists_kernel(dims, *refs):
    nr, nc, capacity, caps, cap, tile_width = dims
    xs, xc, ss, sc, x = refs[:5]
    outs = refs[5 : 5 + nr]
    own, near, far, count, table, picks = refs[5 + nr :]
    group = tile_width // RB
    r, c = lax.axis_index("row"), lax.axis_index("col")

    def clear(i, carry):
        table[i] = 0
        return carry

    lax.fori_loop(0, RB * tile_width, clear, 0, unroll=16)

    def fill(rho, keep):
        live = xc[rho, c]
        for s in reversed(range(capacity)):
            table[xs[rho, c, s]] = jnp.where(s < live, s + 1, 0) if keep else 0

    def scan(rho, target, visit_near, visit_far, state):
        for t in range(caps):
            o = ss[target, c, t]
            base = o // JW * tile_width
            j = jnp.where(t < sc[target, c], o % JW, -1)
            for q in range(group):
                cw = rho * group + q
                for a in range(CAPW):
                    p = xs[target, cw, a]
                    slot = table[base + q * RB + p // tile_width]
                    hit = (p % tile_width == j) & (a < xc[target, cw]) & (slot > 0)
                    state = visit_near(state, hit, slot, t, cw * CAPW + a)
                for v in range(caps):
                    p = ss[target, cw, v]
                    slot = table[base + q * RB + p // JW]
                    hit = (p % JW == j) & (v < sc[target, cw]) & (slot > 0)
                    state = visit_far(state, hit, slot, t, cw * caps + v)
        return state

    for e in range(nr):
        rho = origin(r, e, nr)
        fill(rho, True)

        def note(which, e):
            def visit(state, hit, slot, t, right):
                total, n_near, n_far = state
                take = (hit & (total < cap)).astype(jnp.int32)
                code = total + 64 * t + 256 * right
                if which == 0:
                    near[e, n_near] = code
                    n_near = n_near + take
                else:
                    far[e, n_far] = code
                    n_far = n_far + take
                if e == 0:
                    picks[0, total] = slot - 1
                return total + take, n_near, n_far

            return visit

        zero = jnp.int32(0)
        total, n_near, n_far = scan(rho, r, note(0, e), note(1, e), (zero, zero, zero))
        count[e, 0] = n_near
        count[e, 1] = n_far
        if e == 0:
            totals = [total]
            for k in range(1, nr):

                def pick(state, hit, slot, t, right, k=k):
                    picks[k, state] = slot - 1
                    return state + (hit & (state < cap)).astype(jnp.int32)

                totals.append(scan(r, origin(r, nr - k if not pow2(nr) else k, nr), pick, pick, zero))
            for k in range(nr):

                def copy(n, carry, k=k):
                    outs[k][n] = x[picks[k, n]]
                    return carry

                lax.fori_loop(0, totals[k], copy, 0)
            for t in range(caps):
                o = ss[r, c, t]
                slot = jnp.where(t < sc[r, c], table[o // JW * tile_width + o % JW], 0)

                @pl.when(slot > 0)
                def _():
                    own[t] = x[slot - 1]

                @pl.when(slot <= 0)
                def _():
                    own[t] = jnp.zeros_like(own[t])

        if e < nr - 1:
            fill(rho, False)


def product_kernel(dims, final, *refs):
    nr, nc, per = dims
    codes, count = refs[:2]
    lefts = refs[2 : 2 + nr]
    rights = refs[2 + nr : 2 + nr + nc]
    rest = refs[2 + nr + nc :]
    own = rest[0] if final else None
    out, held, total = rest[-3:]
    c = lax.axis_index("col")
    for k in range(nc):
        me = origin(c, k, nc)
        for a in range(per):
            held[me * per + a] = rights[k][a]
    total[...] = jnp.zeros_like(total)
    for e in range(nr):

        def step(n, carry, e=e):
            code = codes[e, n]
            left = lefts[e][code % 64]
            right = held[code // 256]
            t = code // 64 % 4
            total[t] += jnp.dot(left, right, preferred_element_type=jnp.float32)
            return carry

        lax.fori_loop(0, count[e, 1 if final else 0], step, 0)
    if final:
        out[...] = (1.5 * own[...].astype(jnp.float32) - 0.5 * total[...]).astype(out.dtype)
    else:
        out[...] = total[...].astype(out.dtype)


def smem():
    return pl.BlockSpec(memory_space=pltpu.SMEM)


def vmem():
    return pl.BlockSpec(memory_space=pltpu.VMEM)


def quick(x_blocks, x_slots, x_count, s_slots, s_count, cap):
    nr, nc = lax.axis_size("row"), lax.axis_size("col")
    capacity, size = x_blocks.shape[2], x_blocks.shape[3]
    caps = s_slots.shape[2]
    tile_width = RB * nc // nr
    group = tile_width // RB
    tile = x_blocks.reshape(capacity, size, size)
    block = jax.ShapeDtypeStruct
    n_near, n_far = caps * group * CAPW + 1, caps * group * caps + 1
    made = pl.pallas_call(
        lambda *refs: lists_kernel((nr, nc, capacity, caps, cap, tile_width), *refs),
        out_shape=[block((cap, size, size), tile.dtype)] * nr
        + [
            block((caps, size, size), tile.dtype),
            block((nr, n_near), jnp.int32),
            block((nr, n_far), jnp.int32),
            block((nr, 2), jnp.int32),
        ],
        in_specs=[smem()] * 4 + [vmem()],
        out_specs=[vmem()] * (nr + 1) + [smem()] * 3,
        scratch_shapes=[
            pltpu.SMEM((RB * tile_width,), jnp.int32),
            pltpu.SMEM((nr, cap + 1), jnp.int32),
        ],
        name="lists",
    )(x_slots, x_count, s_slots, s_count, tile)
    sends, (own, near, far, count) = made[:nr], made[nr:]
    windows = gather_col(tile[:CAPW], nc)
    lefts = [sends[0]] + [permute(sends[k], "row", k, nr) for k in range(1, nr)]

    def product(final, codes, rights, extra):
        per = rights[0].shape[0]
        return pl.pallas_call(
            lambda *refs: product_kernel((nr, nc, per), final, *refs),
            out_shape=block((caps, size, size), jnp.bfloat16),
            in_specs=[smem()] * 2 + [vmem()] * (nr + nc + len(extra)),
            out_specs=vmem(),
            scratch_shapes=[
                pltpu.VMEM((nc * per, size, size), jnp.bfloat16),
                pltpu.VMEM((caps, size, size), jnp.float32),
            ],
            name="second" if final else "first",
        )(codes, count, *lefts, *rights, *extra)

    square = product(False, near, windows, [])
    result = product(True, far, gather_col(square, nc), [own])
    return square, result


def local(*args):
    x_blocks, x_slots, x_count, s_slots, s_count = args
    nr, nc = lax.axis_size("row"), lax.axis_size("col")
    if nc % nr:
        square, result = general(*args)
    else:
        cap = min(3 * (nc // nr), x_blocks.shape[2])
        longest = longest_list(x_slots, x_count, s_slots, s_count, RB * nc // nr)
        square, result = quick(*args, cap)
        square, result = lax.cond(
            longest > cap, lambda a, s, u: general(*a), lambda a, s, u: (s, u), args, square, result
        )
    return square[None, None], result[None, None]


def solution(mesh):
    spec = P("row", "col", None, None, None)
    return jax.shard_map(
        local,
        mesh=mesh,
        in_specs=(spec, P(), P(), P(), P()),
        out_specs=(spec, spec),
        check_vma=False,
    )
```

```python
import jax
import jax.numpy as jnp
from jax import lax
from jax.experimental import pallas as pl
from jax.experimental.pallas import tpu as pltpu
from jax.sharding import PartitionSpec as P

RB = 8
JW = 2
CAPW = 2


def pow2(n):
    return n & (n - 1) == 0


def partner(i, k, n):
    return i ^ k if pow2(n) else (i + k) % n


def origin(i, k, n):
    return jnp.bitwise_xor(i, k) if pow2(n) else lax.rem(i + (n - k), n)


def permute(x, axis, k, n):
    return lax.ppermute(x, axis, [(i, partner(i, k, n)) for i in range(n)])


def gather_col(x, n):
    parts = [x] + [None] * (n - 1)
    if n >= 4 and pow2(n):
        half = n // 2
        far = permute(x, "col", half, n)
        parts[half] = far
        for k in range(1, half):
            parts[k] = permute(x, "col", k, n)
        for k in range(1, half):
            parts[half + k] = permute(far, "col", k, n)
    else:
        for k in range(1, n):
            parts[k] = permute(x, "col", k, n)
    return parts


def match_index(targets, slot_keys, slot_live):
    matches = (targets[..., None] == slot_keys) & slot_live
    ordinal = jnp.arange(1, slot_keys.shape[0] + 1, dtype=jnp.int32)
    located = jnp.sum(jnp.where(matches, ordinal, 0), axis=-1)
    return jnp.where(located > 0, located - 1, slot_keys.shape[0])


def ordered(parts, me, n):
    stacked = jnp.stack(parts)
    ids = jnp.stack([origin(me, k, n) for k in range(n)])
    order = jnp.argsort(ids)
    return jnp.take(stacked, order, axis=0)


def general(x_blocks, x_slots, x_count, s_slots, s_count):
    nr, nc = lax.axis_size("row"), lax.axis_size("col")
    row_id, col_id = lax.axis_index("row"), lax.axis_index("col")
    capacity, size = x_blocks.shape[2], x_blocks.shape[3]
    order_blocks = RB * nc
    tile_width = order_blocks // nr
    tile = x_blocks[0, 0]
    panel = ordered([tile] + [permute(tile, "row", k, nr) for k in range(1, nr)], row_id, nr)
    stacked = panel.reshape(nr * capacity, size, size)
    padded = jnp.concatenate([stacked, jnp.zeros((1, size, size), stacked.dtype)], axis=0)
    column_slots = x_slots[:, col_id]
    column_count = x_count[:, col_id]
    ordinal = jnp.arange(capacity, dtype=jnp.int32)
    panel_live = (ordinal[None, :] < column_count[:, None]).reshape(-1)
    owners = jnp.arange(nr, dtype=jnp.int32)[:, None]
    panel_keys = (
        column_slots // tile_width * order_blocks + owners * tile_width + column_slots % tile_width
    ).reshape(-1)
    lanes = jnp.arange(RB, dtype=jnp.int32)

    def multiply(values, inner_row, inner_col, usable):
        picked = match_index(
            lanes[None, :] * order_blocks + inner_row[:, None], panel_keys, panel_live
        )

        def one(n, total):
            left = jnp.take(padded, picked[n], axis=0)
            right = jnp.where(usable[n], values[n], jnp.zeros_like(values[n]))
            part = jnp.einsum("rxy,yz->rxz", left, right, preferred_element_type=jnp.float32)
            column = jnp.clip(inner_col[n], 0, JW - 1)
            return total.at[:, column].add(part)

        start = jnp.zeros((RB, JW, size, size), jnp.float32)
        return lax.fori_loop(0, values.shape[0], one, start).reshape(RB * JW, size, size)

    def spread(table, counts, slots, stride):
        owner_ids = jnp.arange(nc, dtype=jnp.int32)[:, None]
        positions = table[:, :slots]
        inner_row = owner_ids * RB + positions // stride
        inner_col = positions % stride
        usable = (jnp.arange(slots, dtype=jnp.int32)[None, :] < counts[:, None]) & (inner_col < JW)
        return inner_row.reshape(-1), inner_col.reshape(-1), usable.reshape(-1)

    def columns(mine):
        parts = [mine] + [permute(mine, "col", k, nc) for k in range(1, nc)]
        return ordered(parts, col_id, nc).reshape(-1, size, size)

    first = multiply(
        columns(tile[:CAPW]), *spread(x_slots[row_id], x_count[row_id], CAPW, tile_width)
    )
    own_slots = s_slots[row_id, col_id]
    own_live = jnp.arange(own_slots.shape[0], dtype=jnp.int32) < s_count[row_id, col_id]
    square = jnp.where(
        own_live[:, None, None], jnp.take(first, own_slots, axis=0), 0.0
    ).astype(jnp.bfloat16)
    second = multiply(
        columns(square), *spread(s_slots[row_id], s_count[row_id], own_slots.shape[0], JW)
    )
    own_keys = own_slots // JW * order_blocks + row_id * tile_width + own_slots % JW
    own_block = jnp.take(padded, match_index(own_keys, panel_keys, panel_live), axis=0)
    combined = 1.5 * own_block.astype(jnp.float32) - 0.5 * jnp.take(second, own_slots, axis=0)
    result = jnp.where(own_live[:, None, None], combined, 0.0).astype(jnp.bfloat16)
    return square, result


BIG = 1 << 20
STEP = 1 << 10


def wants(target, owner, group, tables, dims):
    xs, xc, ss, sc = tables
    caps, tile_width = dims
    near, far = [], []
    for q in range(group):
        cw = owner * group + q
        for a in range(CAPW):
            p = xs[target, cw, a]
            column = jnp.where(a < xc[target, cw], p % tile_width, -1)
            near.append((q * RB + p // tile_width, column, cw * CAPW + a))
        for v in range(caps):
            p = ss[target, v, cw]
            column = jnp.where(v < sc[target, cw], p % JW, -1)
            far.append((q * RB + p // JW, column, cw * caps + v))
    return near, far


def outputs(target, c, tables, dims):
    xs, xc, ss, sc = tables
    caps, tile_width = dims
    found = []
    for t in range(caps):
        o = ss[target, t, c]
        found.append((o // JW * tile_width, jnp.where(t < sc[target, c], o % JW, -2)))
    return found


def fill(table, xs, xc, rho, c, capacity):
    live = xc[rho, c]
    for s in reversed(range(capacity)):
        table[xs[rho, c, s]] = jnp.where(s < live, s + 1, 0)


def unfill(table, xs, rho, c, capacity):
    for s in range(capacity):
        table[xs[rho, c, s]] = 0


def clear(table, size):
    def one(i, carry):
        table[i] = 0
        return carry

    lax.fori_loop(0, size, one, 0, unroll=16)


def send_kernel(sizes, *refs):
    nr, nc, capacity, caps, cap, tile_width = sizes
    tables, x = refs[:4], refs[4]
    outs = refs[5 : 5 + nr]
    own, window, table, picks = refs[5 + nr :]
    group, dims = tile_width // RB, (caps, tile_width)
    xs, xc, ss, sc = tables
    r, c = lax.axis_index("row"), lax.axis_index("col")
    clear(table, RB * tile_width)
    fill(table, xs, xc, r, c, capacity)
    window[...] = x[:CAPW]
    for k in range(nr):
        target = origin(r, k if pow2(nr) else (nr - k) % nr, nr)
        near, far = wants(target, r, group, tables, dims)
        total = jnp.int32(0)
        for base, j in outputs(target, c, tables, dims):
            for inner, column, _ in near + far:
                slot = table[base + inner]
                picks[total] = slot - 1
                total = total + ((column == j) & (slot > 0)).astype(jnp.int32)

        def copy(n, carry, k=k):
            outs[k][n] = x[picks[n]]
            return carry

        lax.fori_loop(0, jnp.minimum(total, cap), copy, 0)
    for t, (base, j) in enumerate(outputs(r, c, tables, dims)):
        slot = jnp.where(j >= 0, table[base + jnp.maximum(j, 0)], 0)
        block = x[jnp.maximum(slot - 1, 0)]
        own[t] = jnp.where(slot > 0, block, jnp.zeros_like(block))


def plan_kernel(sizes, *refs):
    nr, nc, capacity, caps, cap, tile_width = sizes
    tables, slots_ref = refs[:4], refs[4]
    near_ref, far_ref, count, longest, table = refs[5:]
    group, dims = tile_width // RB, (caps, tile_width)
    xs, xc, ss, sc = tables
    r, c = lax.axis_index("row"), lax.axis_index("col")
    clear(table, RB * tile_width)
    mine = outputs(r, c, tables, dims)
    for e in range(nr):
        rho = origin(r, e, nr)
        fill(table, xs, xc, rho, c, capacity)
        near, far = wants(r, rho, group, tables, dims)
        total, n_near, n_far = jnp.int32(0), jnp.int32(0), jnp.int32(0)
        for t, (base, j) in enumerate(mine):
            for inner, column, right in near:
                slot = table[base + inner]
                near_ref[e, n_near] = total + 64 * t + 256 * right
                hit = ((column == j) & (slot > 0)).astype(jnp.int32)
                n_near, total = n_near + hit, total + hit
            for inner, column, right in far:
                slot = table[base + inner]
                far_ref[e, n_far] = total + 64 * t + 256 * right
                hit = ((column == j) & (slot > 0)).astype(jnp.int32)
                n_far, total = n_far + hit, total + hit
        count[e, 0] = n_near
        count[e, 1] = n_far
        if e < nr - 1:
            unfill(table, xs, rho, c, capacity)
    rows = lax.broadcasted_iota(jnp.int32, (nc, capacity), 0)
    lanes = lax.broadcasted_iota(jnp.int32, (nc, capacity), 1)

    def column_of(read):
        made = jnp.zeros((nc, capacity), jnp.int32)
        for i in range(nc):
            made = jnp.where(rows == i, read(i), made)
        return made

    def per_target(target, best):
        keys = []
        for t in range(caps):

            def key(i):
                o = ss[target, t, i]
                return jnp.where(t < sc[target, i], o // JW * tile_width - o % JW * STEP, BIG)

            keys.append(column_of(key))

        def per_owner(rho, best):
            live = lanes < column_of(lambda i: xc[rho, i])
            held = jnp.where(live, slots_ref[rho], -4 * BIG)
            near, far = wants(target, rho, group, tables, dims)
            scalars = [jnp.where(col < 0, -BIG * 8, inn + col * STEP) for inn, col, _ in near + far]
            hits = jnp.zeros((nc, capacity), jnp.int32)
            for key in keys:
                apart = held - key
                for scalar in scalars:
                    hits = hits + (apart == scalar).astype(jnp.int32)
            return jnp.maximum(best, jnp.sum(hits, axis=1, keepdims=True))

        return lax.fori_loop(0, nr, per_owner, best)

    best = lax.fori_loop(0, nr, per_target, jnp.zeros((nc, 1), jnp.int32))
    longest[0] = jnp.max(best)


def product_kernel(sizes, final, *refs):
    nr, nc, per, cap = sizes
    codes, count = refs[:2]
    lefts = refs[2 : 2 + nr]
    rights = refs[2 + nr : 2 + nr + nc]
    rest = refs[2 + nr + nc :]
    out, held, total = rest[-3:]
    c = lax.axis_index("col")
    for k in range(nc):
        held[pl.ds(origin(c, k, nc) * per, per)] = rights[k][...]
    total[...] = jnp.zeros_like(total)
    for e in range(nr):

        def step(n, carry, e=e):
            code = codes[e, n]
            left = lefts[e][jnp.minimum(code % 64, cap - 1)]
            right = held[code // 256]
            t = code // 64 % 4
            total[t] += jnp.dot(left, right, preferred_element_type=jnp.float32)
            return carry

        lax.fori_loop(0, count[e, 1 if final else 0], step, 0)
    if final:
        own = rest[0][...].astype(jnp.float32)
        out[...] = (1.5 * own - 0.5 * total[...]).astype(out.dtype)
    else:
        out[...] = total[...].astype(out.dtype)


def smem():
    return pl.BlockSpec(memory_space=pltpu.SMEM)


def vmem():
    return pl.BlockSpec(memory_space=pltpu.VMEM)


def grant(blocks):
    return pltpu.CompilerParams(vmem_limit_bytes=(blocks + 64) * 32768)


def quick(x_blocks, x_slots, x_count, s_slots, s_count, cap):
    nr, nc = lax.axis_size("row"), lax.axis_size("col")
    capacity, size = x_blocks.shape[2], x_blocks.shape[3]
    caps = s_slots.shape[2]
    tile_width = RB * nc // nr
    group = tile_width // RB
    tile = x_blocks.reshape(capacity, size, size)
    block = jax.ShapeDtypeStruct
    n_near, n_far = caps * group * CAPW + 1, caps * group * caps + 1
    sizes = (nr, nc, capacity, caps, cap, tile_width)
    tables = (x_slots, x_count, s_slots.transpose(0, 2, 1), s_count)
    made = pl.pallas_call(
        lambda *refs: send_kernel(sizes, *refs),
        out_shape=[block((cap, size, size), tile.dtype)] * nr
        + [block((caps, size, size), tile.dtype), block((CAPW, size, size), tile.dtype)],
        in_specs=[smem()] * 4 + [vmem()],
        out_specs=[vmem()] * (nr + 2),
        scratch_shapes=[
            pltpu.SMEM((RB * tile_width,), jnp.int32),
            pltpu.SMEM((n_near + n_far,), jnp.int32),
        ],
        compiler_params=grant(capacity + cap * nr + caps + CAPW),
        name="send",
    )(*tables, tile)
    sends, (own, window) = made[:nr], made[nr:]
    near, far, count, longest = pl.pallas_call(
        lambda *refs: plan_kernel(sizes, *refs),
        out_shape=[
            block((nr, n_near), jnp.int32),
            block((nr, n_far), jnp.int32),
            block((nr, 2), jnp.int32),
            block((1,), jnp.int32),
        ],
        in_specs=[smem()] * 4 + [vmem()],
        out_specs=[smem()] * 4,
        scratch_shapes=[pltpu.SMEM((RB * tile_width,), jnp.int32)],
        compiler_params=grant(0),
        name="plan",
    )(*tables, x_slots)
    windows = gather_col(window, nc)
    lefts = [sends[0]] + [permute(sends[k], "row", k, nr) for k in range(1, nr)]

    def product(final, codes, rights, extra):
        per = rights[0].shape[0]
        return pl.pallas_call(
            lambda *refs: product_kernel((nr, nc, per, cap), final, *refs),
            out_shape=block((caps, size, size), jnp.bfloat16),
            in_specs=[smem()] * 2 + [vmem()] * (nr + nc + len(extra)),
            out_specs=vmem(),
            scratch_shapes=[
                pltpu.VMEM((nc * per, size, size), jnp.bfloat16),
                pltpu.VMEM((caps, size, size), jnp.float32),
            ],
            compiler_params=grant(cap * nr + 2 * nc * per + 4 * caps),
            name="second" if final else "first",
        )(codes, count, *lefts, *rights, *extra)

    square = product(False, near, windows, [])
    result = product(True, far, gather_col(square, nc), [own])
    return square, result, longest[0]


def local(*args):
    nr, nc = lax.axis_size("row"), lax.axis_size("col")
    if nc % nr:
        square, result = general(*args)
    else:
        cap = min(3 * (nc // nr), args[0].shape[2])
        square, result, longest = quick(*args, cap)
        square, result = lax.cond(
            longest > cap, lambda a, s, u: general(*a), lambda a, s, u: (s, u), args, square, result
        )
    return square[None, None], result[None, None]


def solution(mesh):
    spec = P("row", "col", None, None, None)
    return jax.shard_map(
        local,
        mesh=mesh,
        in_specs=(spec, P(), P(), P(), P()),
        out_specs=(spec, spec),
        check_vma=False,
    )
```

```python
import jax
import jax.numpy as jnp
from jax import lax
from jax.experimental import pallas as pl
from jax.experimental.pallas import tpu as pltpu
from jax.sharding import PartitionSpec as P

RB = 8
JW = 2
CAPW = 2


def pow2(n):
    return n & (n - 1) == 0


def partner(i, k, n):
    return i ^ k if pow2(n) else (i + k) % n


def origin(i, k, n):
    return jnp.bitwise_xor(i, k) if pow2(n) else lax.rem(i + (n - k), n)


def permute(x, axis, k, n):
    return lax.ppermute(x, axis, [(i, partner(i, k, n)) for i in range(n)])


def gather_col(x, n):
    parts = [x] + [None] * (n - 1)
    if n >= 4 and pow2(n):
        half = n // 2
        far = permute(x, "col", half, n)
        parts[half] = far
        for k in range(1, half):
            parts[k] = permute(x, "col", k, n)
        for k in range(1, half):
            parts[half + k] = permute(far, "col", k, n)
    else:
        for k in range(1, n):
            parts[k] = permute(x, "col", k, n)
    return parts


def match_index(targets, slot_keys, slot_live):
    matches = (targets[..., None] == slot_keys) & slot_live
    ordinal = jnp.arange(1, slot_keys.shape[0] + 1, dtype=jnp.int32)
    located = jnp.sum(jnp.where(matches, ordinal, 0), axis=-1)
    return jnp.where(located > 0, located - 1, slot_keys.shape[0])


def ordered(parts, me, n):
    stacked = jnp.stack(parts)
    ids = jnp.stack([origin(me, k, n) for k in range(n)])
    order = jnp.argsort(ids)
    return jnp.take(stacked, order, axis=0)


def general(x_blocks, x_slots, x_count, s_slots, s_count):
    nr, nc = lax.axis_size("row"), lax.axis_size("col")
    row_id, col_id = lax.axis_index("row"), lax.axis_index("col")
    capacity, size = x_blocks.shape[2], x_blocks.shape[3]
    order_blocks = RB * nc
    tile_width = order_blocks // nr
    tile = x_blocks[0, 0]
    panel = ordered([tile] + [permute(tile, "row", k, nr) for k in range(1, nr)], row_id, nr)
    stacked = panel.reshape(nr * capacity, size, size)
    padded = jnp.concatenate([stacked, jnp.zeros((1, size, size), stacked.dtype)], axis=0)
    column_slots = x_slots[:, col_id]
    column_count = x_count[:, col_id]
    ordinal = jnp.arange(capacity, dtype=jnp.int32)
    panel_live = (ordinal[None, :] < column_count[:, None]).reshape(-1)
    owners = jnp.arange(nr, dtype=jnp.int32)[:, None]
    panel_keys = (
        column_slots // tile_width * order_blocks + owners * tile_width + column_slots % tile_width
    ).reshape(-1)
    lanes = jnp.arange(RB, dtype=jnp.int32)

    def multiply(values, inner_row, inner_col, usable):
        picked = match_index(
            lanes[None, :] * order_blocks + inner_row[:, None], panel_keys, panel_live
        )

        def one(n, total):
            left = jnp.take(padded, picked[n], axis=0)
            right = jnp.where(usable[n], values[n], jnp.zeros_like(values[n]))
            part = jnp.einsum("rxy,yz->rxz", left, right, preferred_element_type=jnp.float32)
            column = jnp.clip(inner_col[n], 0, JW - 1)
            return total.at[:, column].add(part)

        start = jnp.zeros((RB, JW, size, size), jnp.float32)
        return lax.fori_loop(0, values.shape[0], one, start).reshape(RB * JW, size, size)

    def spread(table, counts, slots, stride):
        owner_ids = jnp.arange(nc, dtype=jnp.int32)[:, None]
        positions = table[:, :slots]
        inner_row = owner_ids * RB + positions // stride
        inner_col = positions % stride
        usable = (jnp.arange(slots, dtype=jnp.int32)[None, :] < counts[:, None]) & (inner_col < JW)
        return inner_row.reshape(-1), inner_col.reshape(-1), usable.reshape(-1)

    def columns(mine):
        parts = [mine] + [permute(mine, "col", k, nc) for k in range(1, nc)]
        return ordered(parts, col_id, nc).reshape(-1, size, size)

    first = multiply(
        columns(tile[:CAPW]), *spread(x_slots[row_id], x_count[row_id], CAPW, tile_width)
    )
    own_slots = s_slots[row_id, col_id]
    own_live = jnp.arange(own_slots.shape[0], dtype=jnp.int32) < s_count[row_id, col_id]
    square = jnp.where(
        own_live[:, None, None], jnp.take(first, own_slots, axis=0), 0.0
    ).astype(jnp.bfloat16)
    second = multiply(
        columns(square), *spread(s_slots[row_id], s_count[row_id], own_slots.shape[0], JW)
    )
    own_keys = own_slots // JW * order_blocks + row_id * tile_width + own_slots % JW
    own_block = jnp.take(padded, match_index(own_keys, panel_keys, panel_live), axis=0)
    combined = 1.5 * own_block.astype(jnp.float32) - 0.5 * jnp.take(second, own_slots, axis=0)
    result = jnp.where(own_live[:, None, None], combined, 0.0).astype(jnp.bfloat16)
    return square, result


BIG = 1 << 20
STEP = 1 << 10


def wants(target, owner, group, tables, dims):
    xs, xc, ss, sc = tables
    caps, tile_width = dims
    near, far = [], []
    for q in range(group):
        cw = owner * group + q
        for a in range(CAPW):
            p = xs[target, cw, a]
            column = jnp.where(a < xc[target, cw], p % tile_width, -1)
            near.append((q * RB + p // tile_width, column, cw * CAPW + a))
        for v in range(caps):
            p = ss[target, v, cw]
            column = jnp.where(v < sc[target, cw], p % JW, -1)
            far.append((q * RB + p // JW, column, cw * caps + v))
    return near, far


def outputs(target, c, tables, dims):
    xs, xc, ss, sc = tables
    caps, tile_width = dims
    found = []
    for t in range(caps):
        o = ss[target, t, c]
        found.append((o // JW * tile_width, jnp.where(t < sc[target, c], o % JW, -2)))
    return found


def fill(table, xs, xc, rho, c, capacity):
    live = xc[rho, c]
    for s in reversed(range(capacity)):
        table[xs[rho, c, s]] = jnp.where(s < live, s + 1, 0)


def unfill(table, xs, rho, c, capacity):
    for s in range(capacity):
        table[xs[rho, c, s]] = 0


def clear(table, size):
    def one(i, carry):
        table[i] = 0
        return carry

    lax.fori_loop(0, size, one, 0, unroll=16)


def send_kernel(sizes, *refs):
    nr, nc, capacity, caps, cap, tile_width = sizes
    tables, x = refs[:4], refs[4]
    outs = refs[5 : 5 + nr]
    own, window, table, picks = refs[5 + nr :]
    group, dims = tile_width // RB, (caps, tile_width)
    xs, xc, ss, sc = tables
    r, c = lax.axis_index("row"), lax.axis_index("col")
    clear(table, RB * tile_width)
    fill(table, xs, xc, r, c, capacity)
    window[...] = x[:CAPW]
    for k in range(nr):
        target = origin(r, k if pow2(nr) else (nr - k) % nr, nr)
        near, far = wants(target, r, group, tables, dims)
        total = jnp.int32(0)
        for base, j in outputs(target, c, tables, dims):
            for inner, column, _ in near + far:
                slot = table[base + inner]
                picks[total] = slot - 1
                total = total + ((column == j) & (slot > 0)).astype(jnp.int32)

        def copy(n, carry, k=k):
            outs[k][n] = x[picks[n]]
            return carry

        lax.fori_loop(0, jnp.minimum(total, cap), copy, 0)
    for t, (base, j) in enumerate(outputs(r, c, tables, dims)):
        slot = jnp.where(j >= 0, table[base + jnp.maximum(j, 0)], 0)
        block = x[jnp.maximum(slot - 1, 0)]
        own[t] = jnp.where(slot > 0, block, jnp.zeros_like(block))


def plan_kernel(sizes, *refs):
    nr, nc, capacity, caps, cap, tile_width = sizes
    tables = refs[:4]
    near_ref, far_ref, count, table = refs[4:]
    group, dims = tile_width // RB, (caps, tile_width)
    xs, xc, ss, sc = tables
    r, c = lax.axis_index("row"), lax.axis_index("col")
    clear(table, RB * tile_width)
    mine = outputs(r, c, tables, dims)
    for e in range(nr):
        rho = origin(r, e, nr)
        fill(table, xs, xc, rho, c, capacity)
        near, far = wants(r, rho, group, tables, dims)
        total, n_near, n_far = jnp.int32(0), jnp.int32(0), jnp.int32(0)
        for t, (base, j) in enumerate(mine):
            for inner, column, right in near:
                slot = table[base + inner]
                near_ref[e, n_near] = total + 64 * t + 256 * right
                hit = ((column == j) & (slot > 0)).astype(jnp.int32)
                n_near, total = n_near + hit, total + hit
            for inner, column, right in far:
                slot = table[base + inner]
                far_ref[e, n_far] = total + 64 * t + 256 * right
                hit = ((column == j) & (slot > 0)).astype(jnp.int32)
                n_far, total = n_far + hit, total + hit
        count[e, 0] = n_near
        count[e, 1] = n_far
        if e < nr - 1:
            unfill(table, xs, rho, c, capacity)


def count_kernel(sizes, *refs):
    nr, nc, capacity, caps, cap, tile_width = sizes
    tables, slots_ref, _, longest = refs[:4], refs[4], refs[5], refs[6]
    group, dims = tile_width // RB, (caps, tile_width)
    xs, xc, ss, sc = tables
    rows = lax.broadcasted_iota(jnp.int32, (nc, capacity), 0)
    lanes = lax.broadcasted_iota(jnp.int32, (nc, capacity), 1)

    def column_of(read):
        made = jnp.zeros((nc, capacity), jnp.int32)
        for i in range(nc):
            made = jnp.where(rows == i, read(i), made)
        return made

    def per_target(target, best):
        keys = []
        for t in range(caps):

            def key(i):
                o = ss[target, t, i]
                return jnp.where(t < sc[target, i], o // JW * tile_width - o % JW * STEP, BIG)

            keys.append(column_of(key))

        def per_owner(rho, best):
            live = lanes < column_of(lambda i: xc[rho, i])
            held = jnp.where(live, slots_ref[rho], -4 * BIG)
            near, far = wants(target, rho, group, tables, dims)
            scalars = [jnp.where(col < 0, -BIG * 8, inn + col * STEP) for inn, col, _ in near + far]
            hits = jnp.zeros((nc, capacity), jnp.int32)
            for key in keys:
                apart = held - key
                for scalar in scalars:
                    hits = hits + (apart == scalar).astype(jnp.int32)
            return jnp.maximum(best, jnp.sum(hits, axis=1, keepdims=True))

        return lax.fori_loop(0, nr, per_owner, best)

    best = lax.fori_loop(0, nr, per_target, jnp.zeros((nc, 1), jnp.int32))
    longest[0] = jnp.max(best)


def product_kernel(sizes, final, *refs):
    nr, nc, per, cap = sizes
    codes, count = refs[:2]
    lefts = refs[2 : 2 + nr]
    rights = refs[2 + nr : 2 + nr + nc]
    rest = refs[2 + nr + nc :]
    held, total = rest[-2:]
    c = lax.axis_index("col")
    for k in range(nc):
        held[pl.ds(origin(c, k, nc) * per, per)] = rights[k][...]
    total[...] = jnp.zeros_like(total)
    for e in range(nr):

        def step(n, carry, e=e):
            code = codes[e, n]
            left = lefts[e][jnp.minimum(code % 64, cap - 1)]
            right = held[code // 256]
            t = code // 64 % 4
            total[t] += jnp.dot(left, right, preferred_element_type=jnp.float32)
            return carry

        lax.fori_loop(0, count[e, 1 if final else 0], step, 0)
    if final:
        own, out = rest[:2]
        out[...] = (1.5 * own[...].astype(jnp.float32) - 0.5 * total[...]).astype(out.dtype)
    else:
        for out in rest[:2]:
            out[...] = total[...].astype(out.dtype)


def smem():
    return pl.BlockSpec(memory_space=pltpu.SMEM)


def vmem():
    return pl.BlockSpec(memory_space=pltpu.VMEM)


def grant(blocks):
    return pltpu.CompilerParams(vmem_limit_bytes=(blocks + 64) * 32768)


def quick(x_blocks, x_slots, x_count, s_slots, s_count, cap):
    nr, nc = lax.axis_size("row"), lax.axis_size("col")
    capacity, size = x_blocks.shape[2], x_blocks.shape[3]
    caps = s_slots.shape[2]
    tile_width = RB * nc // nr
    group = tile_width // RB
    tile = x_blocks.reshape(capacity, size, size)
    block = jax.ShapeDtypeStruct
    n_near, n_far = caps * group * CAPW + 1, caps * group * caps + 1
    sizes = (nr, nc, capacity, caps, cap, tile_width)
    tables = (x_slots, x_count, s_slots.transpose(0, 2, 1), s_count)
    made = pl.pallas_call(
        lambda *refs: send_kernel(sizes, *refs),
        out_shape=[block((cap, size, size), tile.dtype)] * nr
        + [block((caps, size, size), tile.dtype), block((CAPW, size, size), tile.dtype)],
        in_specs=[smem()] * 4 + [vmem()],
        out_specs=[vmem()] * (nr + 2),
        scratch_shapes=[
            pltpu.SMEM((RB * tile_width,), jnp.int32),
            pltpu.SMEM((n_near + n_far,), jnp.int32),
        ],
        compiler_params=grant(capacity + cap * nr + caps + CAPW),
        name="send",
    )(*tables, tile)
    sends, (own, window) = made[:nr], made[nr:]
    near, far, count = pl.pallas_call(
        lambda *refs: plan_kernel(sizes, *refs),
        out_shape=[
            block((nr, n_near), jnp.int32),
            block((nr, n_far), jnp.int32),
            block((nr, 2), jnp.int32),
        ],
        in_specs=[smem()] * 4,
        out_specs=[smem()] * 3,
        scratch_shapes=[pltpu.SMEM((RB * tile_width,), jnp.int32)],
        compiler_params=grant(0),
        name="plan",
    )(*tables)
    windows = gather_col(window, nc)
    lefts = [sends[0]] + [permute(sends[k], "row", k, nr) for k in range(1, nr)]

    def product(final, codes, rights, extra):
        per = rights[0].shape[0]
        return pl.pallas_call(
            lambda *refs: product_kernel((nr, nc, per, cap), final, *refs),
            out_shape=[block((caps, size, size), jnp.bfloat16)] * (1 if final else 2),
            in_specs=[smem()] * 2 + [vmem()] * (nr + nc + len(extra)),
            out_specs=[vmem()] * (1 if final else 2),
            scratch_shapes=[
                pltpu.VMEM((nc * per, size, size), jnp.bfloat16),
                pltpu.VMEM((caps, size, size), jnp.float32),
            ],
            compiler_params=grant(cap * nr + 2 * nc * per + 4 * caps),
            name="second" if final else "first",
        )(codes, count, *lefts, *rights, *extra)

    square, message = product(False, near, windows, [])
    longest = pl.pallas_call(
        lambda *refs: count_kernel(sizes, *refs),
        out_shape=block((1,), jnp.int32),
        in_specs=[smem()] * 4 + [vmem(), pl.BlockSpec(memory_space=pl.ANY)],
        out_specs=smem(),
        compiler_params=grant(0),
        name="count",
    )(*tables, x_slots, message)
    (result,) = product(True, far, gather_col(message, nc), [own])
    return square, result, longest[0]


def local(*args):
    nr, nc = lax.axis_size("row"), lax.axis_size("col")
    if nc % nr:
        square, result = general(*args)
    else:
        cap = min(3 * (nc // nr), args[0].shape[2])
        square, result, longest = quick(*args, cap)
        square, result = lax.cond(
            longest > cap, lambda a, s, u: general(*a), lambda a, s, u: (s, u), args, square, result
        )
    return square[None, None], result[None, None]


def solution(mesh):
    spec = P("row", "col", None, None, None)
    return jax.shard_map(
        local,
        mesh=mesh,
        in_specs=(spec, P(), P(), P(), P()),
        out_specs=(spec, spec),
        check_vma=False,
    )
```

```python
import jax
import jax.numpy as jnp
from jax import lax
from jax.experimental import pallas as pl
from jax.experimental.pallas import tpu as pltpu
from jax.sharding import PartitionSpec as P

RB = 8
JW = 2
CAPW = 2


def pow2(n):
    return n & (n - 1) == 0


def partner(i, k, n):
    return i ^ k if pow2(n) else (i + k) % n


def origin(i, k, n):
    return jnp.bitwise_xor(i, k) if pow2(n) else lax.rem(i + (n - k), n)


def permute(x, axis, k, n):
    return lax.ppermute(x, axis, [(i, partner(i, k, n)) for i in range(n)])


def col_order(n):
    if n < 4 or not pow2(n):
        return list(range(n))
    half = n // 2
    near = sorted(range(1, half), key=lambda k: (-k.bit_count(), k))
    return [0, half] + near + [half + k for k in near]


def gather_col(x, n):
    half = n // 2
    parts = {0: x}
    for k in col_order(n)[1:]:
        relayed = n >= 4 and pow2(n) and k > half
        parts[k] = permute(parts[half] if relayed else x, "col", k - half if relayed else k, n)
    return list(parts.values())


def match_index(targets, slot_keys, slot_live):
    matches = (targets[..., None] == slot_keys) & slot_live
    ordinal = jnp.arange(1, slot_keys.shape[0] + 1, dtype=jnp.int32)
    located = jnp.sum(jnp.where(matches, ordinal, 0), axis=-1)
    return jnp.where(located > 0, located - 1, slot_keys.shape[0])


def ordered(parts, me, n):
    stacked = jnp.stack(parts)
    ids = jnp.stack([origin(me, k, n) for k in range(n)])
    order = jnp.argsort(ids)
    return jnp.take(stacked, order, axis=0)


def general(x_blocks, x_slots, x_count, s_slots, s_count):
    nr, nc = lax.axis_size("row"), lax.axis_size("col")
    row_id, col_id = lax.axis_index("row"), lax.axis_index("col")
    capacity, size = x_blocks.shape[2], x_blocks.shape[3]
    order_blocks = RB * nc
    tile_width = order_blocks // nr
    tile = x_blocks[0, 0]
    panel = ordered([tile] + [permute(tile, "row", k, nr) for k in range(1, nr)], row_id, nr)
    stacked = panel.reshape(nr * capacity, size, size)
    padded = jnp.concatenate([stacked, jnp.zeros((1, size, size), stacked.dtype)], axis=0)
    column_slots = x_slots[:, col_id]
    column_count = x_count[:, col_id]
    ordinal = jnp.arange(capacity, dtype=jnp.int32)
    panel_live = (ordinal[None, :] < column_count[:, None]).reshape(-1)
    owners = jnp.arange(nr, dtype=jnp.int32)[:, None]
    panel_keys = (
        column_slots // tile_width * order_blocks + owners * tile_width + column_slots % tile_width
    ).reshape(-1)
    lanes = jnp.arange(RB, dtype=jnp.int32)

    def multiply(values, inner_row, inner_col, usable):
        picked = match_index(
            lanes[None, :] * order_blocks + inner_row[:, None], panel_keys, panel_live
        )

        def one(n, total):
            left = jnp.take(padded, picked[n], axis=0)
            right = jnp.where(usable[n], values[n], jnp.zeros_like(values[n]))
            part = jnp.einsum("rxy,yz->rxz", left, right, preferred_element_type=jnp.float32)
            column = jnp.clip(inner_col[n], 0, JW - 1)
            return total.at[:, column].add(part)

        start = jnp.zeros((RB, JW, size, size), jnp.float32)
        return lax.fori_loop(0, values.shape[0], one, start).reshape(RB * JW, size, size)

    def spread(table, counts, slots, stride):
        owner_ids = jnp.arange(nc, dtype=jnp.int32)[:, None]
        positions = table[:, :slots]
        inner_row = owner_ids * RB + positions // stride
        inner_col = positions % stride
        usable = (jnp.arange(slots, dtype=jnp.int32)[None, :] < counts[:, None]) & (inner_col < JW)
        return inner_row.reshape(-1), inner_col.reshape(-1), usable.reshape(-1)

    def columns(mine):
        parts = [mine] + [permute(mine, "col", k, nc) for k in range(1, nc)]
        return ordered(parts, col_id, nc).reshape(-1, size, size)

    first = multiply(
        columns(tile[:CAPW]), *spread(x_slots[row_id], x_count[row_id], CAPW, tile_width)
    )
    own_slots = s_slots[row_id, col_id]
    own_live = jnp.arange(own_slots.shape[0], dtype=jnp.int32) < s_count[row_id, col_id]
    square = jnp.where(
        own_live[:, None, None], jnp.take(first, own_slots, axis=0), 0.0
    ).astype(jnp.bfloat16)
    second = multiply(
        columns(square), *spread(s_slots[row_id], s_count[row_id], own_slots.shape[0], JW)
    )
    own_keys = own_slots // JW * order_blocks + row_id * tile_width + own_slots % JW
    own_block = jnp.take(padded, match_index(own_keys, panel_keys, panel_live), axis=0)
    combined = 1.5 * own_block.astype(jnp.float32) - 0.5 * jnp.take(second, own_slots, axis=0)
    result = jnp.where(own_live[:, None, None], combined, 0.0).astype(jnp.bfloat16)
    return square, result


BIG = 1 << 20
STEP = 1 << 10


def wants(target, owner, group, tables, dims):
    xs, xc, ss, sc = tables
    caps, tile_width = dims
    near, far = [], []
    for q in range(group):
        cw = owner * group + q
        for a in range(CAPW):
            p = xs[target, cw, a]
            column = jnp.where(a < xc[target, cw], p % tile_width, -1)
            near.append((q * RB + p // tile_width, column, cw * CAPW + a))
        for v in range(caps):
            p = ss[target, v, cw]
            column = jnp.where(v < sc[target, cw], p % JW, -1)
            far.append((q * RB + p // JW, column, cw * caps + v))
    return near, far


def outputs(target, c, tables, dims):
    xs, xc, ss, sc = tables
    caps, tile_width = dims
    found = []
    for t in range(caps):
        o = ss[target, t, c]
        found.append((o // JW * tile_width, jnp.where(t < sc[target, c], o % JW, -2)))
    return found


def fill(table, xs, xc, rho, c, capacity):
    live = xc[rho, c]
    for s in reversed(range(capacity)):
        table[xs[rho, c, s]] = jnp.where(s < live, s + 1, 0)


def unfill(table, xs, rho, c, capacity):
    for s in range(capacity):
        table[xs[rho, c, s]] = 0


def clear(table, size):
    def one(i, carry):
        table[i] = 0
        return carry

    lax.fori_loop(0, size, one, 0, unroll=16)


def send_kernel(sizes, *refs):
    nr, nc, capacity, caps, cap, tile_width = sizes
    tables, x = refs[:4], refs[4]
    outs = refs[5 : 5 + nr]
    own, window, table, picks = refs[5 + nr :]
    group, dims = tile_width // RB, (caps, tile_width)
    xs, xc, ss, sc = tables
    r, c = lax.axis_index("row"), lax.axis_index("col")
    clear(table, RB * tile_width)
    fill(table, xs, xc, r, c, capacity)
    window[...] = x[:CAPW]
    for k in range(nr):
        target = origin(r, k if pow2(nr) else (nr - k) % nr, nr)
        near, far = wants(target, r, group, tables, dims)
        total = jnp.int32(0)
        for base, j in outputs(target, c, tables, dims):
            for inner, column, _ in near + far:
                slot = table[base + inner]
                picks[total] = slot - 1
                total = total + ((column == j) & (slot > 0)).astype(jnp.int32)

        def copy(n, carry, k=k):
            outs[k][n] = x[picks[n]]
            return carry

        lax.fori_loop(0, jnp.minimum(total, cap), copy, 0)
    for t, (base, j) in enumerate(outputs(r, c, tables, dims)):
        slot = jnp.where(j >= 0, table[base + jnp.maximum(j, 0)], 0)
        block = x[jnp.maximum(slot - 1, 0)]
        own[t] = jnp.where(slot > 0, block, jnp.zeros_like(block))


def plan_kernel(sizes, *refs):
    nr, nc, capacity, caps, cap, tile_width = sizes
    tables = refs[:4]
    near_ref, far_ref, count, table = refs[4:]
    group, dims = tile_width // RB, (caps, tile_width)
    xs, xc, ss, sc = tables
    r, c = lax.axis_index("row"), lax.axis_index("col")
    clear(table, RB * tile_width)
    mine = outputs(r, c, tables, dims)
    for e in range(nr):
        rho = origin(r, e, nr)
        fill(table, xs, xc, rho, c, capacity)
        near, far = wants(r, rho, group, tables, dims)
        total, n_near, n_far = jnp.int32(0), jnp.int32(0), jnp.int32(0)
        for t, (base, j) in enumerate(mine):
            for inner, column, right in near:
                slot = table[base + inner]
                near_ref[e, n_near] = total + 64 * t + 256 * right
                hit = ((column == j) & (slot > 0)).astype(jnp.int32)
                n_near, total = n_near + hit, total + hit
            for inner, column, right in far:
                slot = table[base + inner]
                far_ref[e, n_far] = total + 64 * t + 256 * right
                hit = ((column == j) & (slot > 0)).astype(jnp.int32)
                n_far, total = n_far + hit, total + hit
        count[e, 0] = n_near
        count[e, 1] = n_far
        if e < nr - 1:
            unfill(table, xs, rho, c, capacity)


def count_kernel(sizes, *refs):
    nr, nc, capacity, caps, cap, tile_width = sizes
    tables, slots_ref, _, over, hits = refs[:4], refs[4], refs[5], refs[6], refs[7]
    group, dims = tile_width // RB, (caps, tile_width)
    xs, xc, ss, sc = tables
    rows = lax.broadcasted_iota(jnp.int32, (nc, capacity), 0)
    lanes = lax.broadcasted_iota(jnp.int32, (nc, capacity), 1)

    def loop(n, body):
        if n <= 4:
            for i in range(n):
                body(i)
        else:
            lax.fori_loop(0, n, lambda i, carry: body(i) or carry, 0)

    def column_of(read):
        made = jnp.zeros((nc, capacity), jnp.int32)
        for i in range(nc):
            made = jnp.where(rows == i, read(i), made)
        return made

    held_of = [None] * nr
    for rho in range(nr if nr <= 4 else 0):
        live = lanes < column_of(lambda i: xc[rho, i])
        held_of[rho] = jnp.where(live, slots_ref[rho], -4 * BIG)

    def per_target(target):
        keys = []
        for t in range(caps):

            def key(i):
                o = ss[target, t, i]
                return jnp.where(t < sc[target, i], o // JW * tile_width - o % JW * STEP, BIG)

            keys.append(column_of(key))

        def per_owner(rho):
            if nr <= 4:
                held = held_of[rho]
            else:
                live = lanes < column_of(lambda i: xc[rho, i])
                held = jnp.where(live, slots_ref[rho], -4 * BIG)
            near, far = wants(target, rho, group, tables, dims)
            scalars = [jnp.where(col < 0, -BIG * 8, inn + col * STEP) for inn, col, _ in near + far]
            found = jnp.zeros((nc, capacity), jnp.int32)
            for key in keys:
                apart = held - key
                for scalar in scalars:
                    found = found + (apart == scalar).astype(jnp.int32)
            hits[target * nr + rho] = found

        loop(nr, per_owner)

    loop(nr, per_target)
    longest = jnp.max(jnp.sum(hits[...], axis=2))
    over[0] = (longest > cap).astype(jnp.int32)


def product_kernel(sizes, final, *refs):
    nr, nc, per, cap = sizes
    codes, count = refs[:2]
    lefts = refs[2 : 2 + nr]
    rights = refs[2 + nr : 2 + nr + nc]
    rest = refs[2 + nr + nc :]
    held, total = rest[-2:]
    c = lax.axis_index("col")
    for k, right in zip(col_order(nc), rights):
        held[pl.ds(origin(c, k, nc) * per, per)] = right[...]
    total[...] = jnp.zeros_like(total)
    for e in range(nr):

        def step(n, carry, e=e):
            code = codes[e, n]
            left = lefts[e][jnp.minimum(code % 64, cap - 1)]
            right = held[code // 256]
            t = code // 64 % 4
            total[t] += jnp.dot(left, right, preferred_element_type=jnp.float32)
            return carry

        lax.fori_loop(0, count[e, 1 if final else 0], step, 0)
    if final:
        own, out = rest[:2]
        out[...] = (1.5 * own[...].astype(jnp.float32) - 0.5 * total[...]).astype(out.dtype)
    else:
        for out in rest[:2]:
            out[...] = total[...].astype(out.dtype)


def smem():
    return pl.BlockSpec(memory_space=pltpu.SMEM)


def vmem():
    return pl.BlockSpec(memory_space=pltpu.VMEM)


def grant(blocks):
    return pltpu.CompilerParams(vmem_limit_bytes=(blocks + 64) * 32768)


def quick(x_blocks, x_slots, x_count, s_slots, s_count, cap):
    nr, nc = lax.axis_size("row"), lax.axis_size("col")
    capacity, size = x_blocks.shape[2], x_blocks.shape[3]
    caps = s_slots.shape[2]
    tile_width = RB * nc // nr
    group = tile_width // RB
    tile = x_blocks.reshape(capacity, size, size)
    block = jax.ShapeDtypeStruct
    n_near, n_far = caps * group * CAPW + 1, caps * group * caps + 1
    sizes = (nr, nc, capacity, caps, cap, tile_width)
    tables = (x_slots, x_count, s_slots.transpose(0, 2, 1), s_count)
    made = pl.pallas_call(
        lambda *refs: send_kernel(sizes, *refs),
        out_shape=[block((cap, size, size), tile.dtype)] * nr
        + [block((caps, size, size), tile.dtype), block((CAPW, size, size), tile.dtype)],
        in_specs=[smem()] * 4 + [vmem()],
        out_specs=[vmem()] * (nr + 2),
        scratch_shapes=[
            pltpu.SMEM((RB * tile_width,), jnp.int32),
            pltpu.SMEM((n_near + n_far,), jnp.int32),
        ],
        compiler_params=grant(capacity + cap * nr + caps + CAPW),
        name="send",
    )(*tables, tile)
    sends, (own, window) = made[:nr], made[nr:]
    near, far, count = pl.pallas_call(
        lambda *refs: plan_kernel(sizes, *refs),
        out_shape=[
            block((nr, n_near), jnp.int32),
            block((nr, n_far), jnp.int32),
            block((nr, 2), jnp.int32),
        ],
        in_specs=[smem()] * 4,
        out_specs=[smem()] * 3,
        scratch_shapes=[pltpu.SMEM((RB * tile_width,), jnp.int32)],
        compiler_params=grant(0),
        name="plan",
    )(*tables)
    windows = gather_col(window, nc)
    lefts = [sends[0]] + [permute(sends[k], "row", k, nr) for k in range(1, nr)]

    def product(final, codes, rights, extra):
        per = rights[0].shape[0]
        return pl.pallas_call(
            lambda *refs: product_kernel((nr, nc, per, cap), final, *refs),
            out_shape=[block((caps, size, size), jnp.bfloat16)] * (1 if final else 2),
            in_specs=[smem()] * 2 + [vmem()] * (nr + nc + len(extra)),
            out_specs=[vmem()] * (1 if final else 2),
            scratch_shapes=[
                pltpu.VMEM((nc * per, size, size), jnp.bfloat16),
                pltpu.VMEM((caps, size, size), jnp.float32),
            ],
            compiler_params=grant(cap * nr + 2 * nc * per + 4 * caps),
            name="second" if final else "first",
        )(codes, count, *lefts, *rights, *extra)

    square, message = product(False, near, windows, [])
    over = pl.pallas_call(
        lambda *refs: count_kernel(sizes, *refs),
        out_shape=block((1,), jnp.int32),
        in_specs=[smem()] * 4 + [vmem(), pl.BlockSpec(memory_space=pl.ANY)],
        out_specs=smem(),
        scratch_shapes=[pltpu.VMEM((nr * nr, nc, capacity), jnp.int32)],
        compiler_params=grant(0),
        name="count",
    )(*tables, x_slots, message)
    (result,) = product(True, far, gather_col(message, nc), [own])
    return square, result, over[0]


def local(*args):
    nr, nc = lax.axis_size("row"), lax.axis_size("col")
    if nc % nr:
        square, result = general(*args)
    else:
        cap = min(3 * (nc // nr), args[0].shape[2])
        square, result, over = quick(*args, cap)
        square, result = lax.cond(
            over > 0, lambda a, s, u: general(*a), lambda a, s, u: (s, u), args, square, result
        )
    return square[None, None], result[None, None]


def solution(mesh):
    spec = P("row", "col", None, None, None)
    return jax.shard_map(
        local,
        mesh=mesh,
        in_specs=(spec, P(), P(), P(), P()),
        out_specs=(spec, spec),
        check_vma=False,
    )
```

```python
import jax
import jax.numpy as jnp
from jax import lax
from jax.experimental import pallas as pl
from jax.experimental.pallas import tpu as pltpu
from jax.sharding import PartitionSpec as P

RB = 8
JW = 2
CAPW = 2
EARLY = (3,)


def pow2(n):
    return n & (n - 1) == 0


def partner(i, k, n):
    return i ^ k if pow2(n) else (i + k) % n


def origin(i, k, n):
    return jnp.bitwise_xor(i, k) if pow2(n) else lax.rem(i + (n - k), n)


def permute(x, axis, k, n):
    return lax.ppermute(x, axis, [(i, partner(i, k, n)) for i in range(n)])


def col_order(n):
    if n < 4 or not pow2(n):
        return list(range(n))
    half = n // 2
    near = sorted(range(1, half), key=lambda k: (-k.bit_count(), k))
    return [0, half] + near + [half + k for k in near]


def gather_col(x, n):
    half = n // 2
    parts = {0: x}
    for k in col_order(n)[1:]:
        relayed = n >= 4 and pow2(n) and k > half
        parts[k] = permute(parts[half] if relayed else x, "col", k - half if relayed else k, n)
    return [((k,), part) for k, part in parts.items()]


def gather_col_joined(x, n, early):
    if n < 4 or not pow2(n):
        return gather_col(x, n)
    half = n // 2
    far = permute(x, "col", half, n)
    near = col_order(n)[2 : 1 + half]
    alone = [((k,), permute(x, "col", k, n)) for k in near if k in early]
    both = jnp.concatenate([x, far])
    parts = [((0, half), both)] + alone
    for k in near:
        if k in early:
            parts.append(((half + k,), permute(far, "col", k, n)))
        else:
            parts.append(((k, half + k), permute(both, "col", k, n)))
    return parts


def match_index(targets, slot_keys, slot_live):
    matches = (targets[..., None] == slot_keys) & slot_live
    ordinal = jnp.arange(1, slot_keys.shape[0] + 1, dtype=jnp.int32)
    located = jnp.sum(jnp.where(matches, ordinal, 0), axis=-1)
    return jnp.where(located > 0, located - 1, slot_keys.shape[0])


def ordered(parts, me, n):
    stacked = jnp.stack(parts)
    ids = jnp.stack([origin(me, k, n) for k in range(n)])
    order = jnp.argsort(ids)
    return jnp.take(stacked, order, axis=0)


def general(x_blocks, x_slots, x_count, s_slots, s_count):
    nr, nc = lax.axis_size("row"), lax.axis_size("col")
    row_id, col_id = lax.axis_index("row"), lax.axis_index("col")
    capacity, size = x_blocks.shape[2], x_blocks.shape[3]
    order_blocks = RB * nc
    tile_width = order_blocks // nr
    tile = x_blocks[0, 0]
    panel = ordered([tile] + [permute(tile, "row", k, nr) for k in range(1, nr)], row_id, nr)
    stacked = panel.reshape(nr * capacity, size, size)
    padded = jnp.concatenate([stacked, jnp.zeros((1, size, size), stacked.dtype)], axis=0)
    column_slots = x_slots[:, col_id]
    column_count = x_count[:, col_id]
    ordinal = jnp.arange(capacity, dtype=jnp.int32)
    panel_live = (ordinal[None, :] < column_count[:, None]).reshape(-1)
    owners = jnp.arange(nr, dtype=jnp.int32)[:, None]
    panel_keys = (
        column_slots // tile_width * order_blocks + owners * tile_width + column_slots % tile_width
    ).reshape(-1)
    lanes = jnp.arange(RB, dtype=jnp.int32)

    def multiply(values, inner_row, inner_col, usable):
        picked = match_index(
            lanes[None, :] * order_blocks + inner_row[:, None], panel_keys, panel_live
        )

        def one(n, total):
            left = jnp.take(padded, picked[n], axis=0)
            right = jnp.where(usable[n], values[n], jnp.zeros_like(values[n]))
            part = jnp.einsum("rxy,yz->rxz", left, right, preferred_element_type=jnp.float32)
            column = jnp.clip(inner_col[n], 0, JW - 1)
            return total.at[:, column].add(part)

        start = jnp.zeros((RB, JW, size, size), jnp.float32)
        return lax.fori_loop(0, values.shape[0], one, start).reshape(RB * JW, size, size)

    def spread(table, counts, slots, stride):
        owner_ids = jnp.arange(nc, dtype=jnp.int32)[:, None]
        positions = table[:, :slots]
        inner_row = owner_ids * RB + positions // stride
        inner_col = positions % stride
        usable = (jnp.arange(slots, dtype=jnp.int32)[None, :] < counts[:, None]) & (inner_col < JW)
        return inner_row.reshape(-1), inner_col.reshape(-1), usable.reshape(-1)

    def columns(mine):
        parts = [mine] + [permute(mine, "col", k, nc) for k in range(1, nc)]
        return ordered(parts, col_id, nc).reshape(-1, size, size)

    first = multiply(
        columns(tile[:CAPW]), *spread(x_slots[row_id], x_count[row_id], CAPW, tile_width)
    )
    own_slots = s_slots[row_id, col_id]
    own_live = jnp.arange(own_slots.shape[0], dtype=jnp.int32) < s_count[row_id, col_id]
    square = jnp.where(
        own_live[:, None, None], jnp.take(first, own_slots, axis=0), 0.0
    ).astype(jnp.bfloat16)
    second = multiply(
        columns(square), *spread(s_slots[row_id], s_count[row_id], own_slots.shape[0], JW)
    )
    own_keys = own_slots // JW * order_blocks + row_id * tile_width + own_slots % JW
    own_block = jnp.take(padded, match_index(own_keys, panel_keys, panel_live), axis=0)
    combined = 1.5 * own_block.astype(jnp.float32) - 0.5 * jnp.take(second, own_slots, axis=0)
    result = jnp.where(own_live[:, None, None], combined, 0.0).astype(jnp.bfloat16)
    return square, result


BIG = 1 << 20
STEP = 1 << 10


def wants(target, owner, group, tables, dims):
    xs, xc, ss, sc = tables
    caps, tile_width = dims
    near, far = [], []
    for q in range(group):
        cw = owner * group + q
        for a in range(CAPW):
            p = xs[target, cw, a]
            column = jnp.where(a < xc[target, cw], p % tile_width, -1)
            near.append((q * RB + p // tile_width, column, cw * CAPW + a))
        for v in range(caps):
            p = ss[target, v, cw]
            column = jnp.where(v < sc[target, cw], p % JW, -1)
            far.append((q * RB + p // JW, column, cw * caps + v))
    return near, far


def outputs(target, c, tables, dims):
    xs, xc, ss, sc = tables
    caps, tile_width = dims
    found = []
    for t in range(caps):
        o = ss[target, t, c]
        found.append((o // JW * tile_width, jnp.where(t < sc[target, c], o % JW, -2)))
    return found


def fill(table, xs, xc, rho, c, capacity):
    live = xc[rho, c]
    for s in reversed(range(capacity)):
        table[xs[rho, c, s]] = jnp.where(s < live, s + 1, 0)


def unfill(table, xs, rho, c, capacity):
    for s in range(capacity):
        table[xs[rho, c, s]] = 0


def clear(table, size):
    def one(i, carry):
        table[i] = 0
        return carry

    lax.fori_loop(0, size, one, 0, unroll=16)


def send_kernel(sizes, *refs):
    nr, nc, capacity, caps, limits, tile_width = sizes
    tables, x = refs[:4], refs[4]
    outs = refs[5 : 5 + nr]
    own, table, picks = refs[5 + nr :]
    group, dims = tile_width // RB, (caps, tile_width)
    xs, xc, ss, sc = tables
    r, c = lax.axis_index("row"), lax.axis_index("col")
    clear(table, RB * tile_width)
    fill(table, xs, xc, r, c, capacity)
    for k in range(nr):
        target = origin(r, k if pow2(nr) else (nr - k) % nr, nr)
        near, far = wants(target, r, group, tables, dims)
        total = jnp.int32(0)
        for base, j in outputs(target, c, tables, dims):
            for inner, column, _ in near + far:
                slot = table[base + inner]
                picks[total] = slot - 1
                total = total + ((column == j) & (slot > 0)).astype(jnp.int32)

        def copy(n, carry, k=k):
            outs[k][n] = x[picks[n]]
            return carry

        lax.fori_loop(0, jnp.minimum(total, limits[k]), copy, 0)
    for t, (base, j) in enumerate(outputs(r, c, tables, dims)):
        slot = jnp.where(j >= 0, table[base + jnp.maximum(j, 0)], 0)
        block = x[jnp.maximum(slot - 1, 0)]
        own[t] = jnp.where(slot > 0, block, jnp.zeros_like(block))


def plan_kernel(sizes, *refs):
    nr, nc, capacity, caps, limits, tile_width = sizes
    tables = refs[:4]
    near_ref, far_ref, count, table = refs[4:]
    group, dims = tile_width // RB, (caps, tile_width)
    xs, xc, ss, sc = tables
    r, c = lax.axis_index("row"), lax.axis_index("col")
    clear(table, RB * tile_width)
    mine = outputs(r, c, tables, dims)
    for e in range(nr):
        rho = origin(r, e, nr)
        fill(table, xs, xc, rho, c, capacity)
        near, far = wants(r, rho, group, tables, dims)
        total, n_near, n_far = jnp.int32(0), jnp.int32(0), jnp.int32(0)
        for t, (base, j) in enumerate(mine):
            for inner, column, right in near:
                slot = table[base + inner]
                near_ref[e, n_near] = total + 64 * t + 256 * right
                hit = ((column == j) & (slot > 0)).astype(jnp.int32)
                n_near, total = n_near + hit, total + hit
            for inner, column, right in far:
                slot = table[base + inner]
                far_ref[e, n_far] = total + 64 * t + 256 * right
                hit = ((column == j) & (slot > 0)).astype(jnp.int32)
                n_far, total = n_far + hit, total + hit
        count[e, 0] = n_near
        count[e, 1] = n_far
        if e < nr - 1:
            unfill(table, xs, rho, c, capacity)


def count_kernel(sizes, *refs):
    nr, nc, capacity, caps, limits, tile_width = sizes
    tables = refs[:4]
    slots_ref, message, over, square, hits, sent = refs[4:]
    sending = pltpu.make_async_copy(message, square, sent)
    sending.start()
    group, dims = tile_width // RB, (caps, tile_width)
    xs, xc, ss, sc = tables
    rows = lax.broadcasted_iota(jnp.int32, (nc, capacity), 0)
    lanes = lax.broadcasted_iota(jnp.int32, (nc, capacity), 1)

    def loop(n, body):
        if n <= 4:
            for i in range(n):
                body(i)
        else:
            lax.fori_loop(0, n, lambda i, carry: body(i) or carry, 0)

    def column_of(read):
        made = jnp.zeros((nc, capacity), jnp.int32)
        for i in range(nc):
            made = jnp.where(rows == i, read(i), made)
        return made

    held_of = [None] * nr
    for rho in range(nr if nr <= 4 else 0):
        live = lanes < column_of(lambda i: xc[rho, i])
        held_of[rho] = jnp.where(live, slots_ref[rho], -4 * BIG)

    def per_target(target):
        keys = []
        for t in range(caps):

            def key(i):
                o = ss[target, t, i]
                return jnp.where(t < sc[target, i], o // JW * tile_width - o % JW * STEP, BIG)

            keys.append(column_of(key))

        def per_owner(rho):
            if nr <= 4:
                held = held_of[rho]
            else:
                live = lanes < column_of(lambda i: xc[rho, i])
                held = jnp.where(live, slots_ref[rho], -4 * BIG)
            near, far = wants(target, rho, group, tables, dims)
            scalars = [jnp.where(col < 0, -BIG * 8, inn + col * STEP) for inn, col, _ in near + far]
            found = jnp.zeros((nc, capacity), jnp.int32)
            for key in keys:
                apart = held - key
                for scalar in scalars:
                    found = found + (apart == scalar).astype(jnp.int32)
            spare = jnp.where(rho == target, limits[0], limits[1])
            hits[target * nr + rho] = jnp.where(lanes == 0, found - spare, found)

        loop(nr, per_owner)

    loop(nr, per_target)
    longest = jnp.max(jnp.sum(hits[...], axis=2))
    over[0] = (longest > 0).astype(jnp.int32)
    sending.wait()


def product_kernel(sizes, final, *refs):
    nr, nc, per, limits, offsets = sizes
    codes, count = refs[:2]
    rights = refs[2 : 2 + len(offsets)]
    lefts = refs[2 + len(offsets) : 2 + len(offsets) + nr]
    rest = refs[2 + len(offsets) + nr :]
    held, total = rest[-2:]
    c = lax.axis_index("col")
    for ks, right in zip(offsets, rights):
        for i, k in enumerate(ks):
            held[pl.ds(origin(c, k, nc) * per, per)] = right[i * per : (i + 1) * per]
    total[...] = jnp.zeros_like(total)
    for e in range(nr):

        def step(n, carry, e=e):
            code = codes[e, n]
            left = lefts[e][jnp.minimum(code % 64, limits[e] - 1)]
            right = held[code // 256]
            t = code // 64 % 4
            total[t] += jnp.dot(left, right, preferred_element_type=jnp.float32)
            return carry

        lax.fori_loop(0, count[e, 1 if final else 0], step, 0)
    if final:
        own, out = rest[:2]
        out[...] = (1.5 * own[...].astype(jnp.float32) - 0.5 * total[...]).astype(out.dtype)
    else:
        rest[0][...] = total[...].astype(rest[0].dtype)


def smem():
    return pl.BlockSpec(memory_space=pltpu.SMEM)


def vmem():
    return pl.BlockSpec(memory_space=pltpu.VMEM)


def grant(blocks):
    return pltpu.CompilerParams(vmem_limit_bytes=(blocks + 64) * 32768)


def quick(x_blocks, x_slots, x_count, s_slots, s_count):
    nr, nc = lax.axis_size("row"), lax.axis_size("col")
    capacity, size = x_blocks.shape[2], x_blocks.shape[3]
    caps = s_slots.shape[2]
    tile_width = RB * nc // nr
    group = tile_width // RB
    tile = x_blocks.reshape(capacity, size, size)
    block = jax.ShapeDtypeStruct
    n_near, n_far = caps * group * CAPW + 1, caps * group * caps + 1
    limits = [min(capacity, 4 * group)] + [min(capacity, 5 * group // 2)] * (nr - 1)
    sizes = (nr, nc, capacity, caps, limits, tile_width)
    tables = (x_slots, x_count, s_slots.transpose(0, 2, 1), s_count)
    made = pl.pallas_call(
        lambda *refs: send_kernel(sizes, *refs),
        out_shape=[block((n, size, size), tile.dtype) for n in limits]
        + [block((caps, size, size), tile.dtype)],
        in_specs=[smem()] * 4 + [vmem()],
        out_specs=[vmem()] * (nr + 1),
        scratch_shapes=[
            pltpu.SMEM((RB * tile_width,), jnp.int32),
            pltpu.SMEM((n_near + n_far,), jnp.int32),
        ],
        compiler_params=grant(capacity + sum(limits) + caps),
        name="send",
    )(*tables, tile)
    sends, own = made[:nr], made[nr]
    near, far, count = pl.pallas_call(
        lambda *refs: plan_kernel(sizes, *refs),
        out_shape=[
            block((nr, n_near), jnp.int32),
            block((nr, n_far), jnp.int32),
            block((nr, 2), jnp.int32),
        ],
        in_specs=[smem()] * 4,
        out_specs=[smem()] * 3,
        scratch_shapes=[pltpu.SMEM((RB * tile_width,), jnp.int32)],
        compiler_params=grant(0),
        name="plan",
    )(*tables)
    windows = gather_col_joined(tile[:CAPW], nc, EARLY)
    lefts = [sends[0]] + [permute(sends[k], "row", k, nr) for k in range(1, nr)]

    def product(final, codes, per, gathered, extra):
        offsets, rights = zip(*gathered)
        return pl.pallas_call(
            lambda *refs: product_kernel((nr, nc, per, limits, offsets), final, *refs),
            out_shape=block((caps, size, size), jnp.bfloat16),
            in_specs=[smem()] * 2 + [vmem()] * (nr + len(rights) + len(extra)),
            out_specs=vmem(),
            scratch_shapes=[
                pltpu.VMEM((nc * per, size, size), jnp.bfloat16),
                pltpu.VMEM((caps, size, size), jnp.float32),
            ],
            compiler_params=grant(sum(limits) + 2 * nc * per + 6 * caps),
            name="second" if final else "first",
        )(codes, count, *rights, *lefts, *extra)

    message = product(False, near, CAPW, windows, [])
    over, square = pl.pallas_call(
        lambda *refs: count_kernel(sizes, *refs),
        out_shape=[block((1,), jnp.int32), block(message.shape, message.dtype)],
        in_specs=[smem()] * 4 + [vmem()] * 2,
        out_specs=[smem(), pl.BlockSpec(memory_space=pltpu.HBM)],
        scratch_shapes=[pltpu.VMEM((nr * nr, nc, capacity), jnp.int32), pltpu.SemaphoreType.DMA],
        compiler_params=grant(2 * caps),
        name="count",
    )(*tables, x_slots, message)
    result = product(True, far, caps, gather_col(message, nc), [own])
    return square, result, over[0]


def local(*args):
    nr, nc = lax.axis_size("row"), lax.axis_size("col")
    if nc % nr:
        square, result = general(*args)
    else:
        square, result, over = quick(*args)
        square, result = lax.cond(
            over > 0, lambda a, s, u: general(*a), lambda a, s, u: (s, u), args, square, result
        )
    return square[None, None], result[None, None]


def solution(mesh):
    spec = P("row", "col", None, None, None)
    return jax.shard_map(
        local,
        mesh=mesh,
        in_specs=(spec, P(), P(), P(), P()),
        out_specs=(spec, spec),
        check_vma=False,
    )
```

```python
import jax
import jax.numpy as jnp
from jax import lax
from jax.experimental import pallas as pl
from jax.experimental.pallas import tpu as pltpu
from jax.sharding import PartitionSpec as P

RB = 8
JW = 2
CAPW = 2


def pow2(n):
    return n & (n - 1) == 0


def partner(i, k, n):
    return i ^ k if pow2(n) else (i + k) % n


def origin(i, k, n):
    return jnp.bitwise_xor(i, k) if pow2(n) else lax.rem(i + (n - k), n)


def permute(x, axis, k, n):
    return lax.ppermute(x, axis, [(i, partner(i, k, n)) for i in range(n)])


def col_order(n):
    if n < 4 or not pow2(n):
        return list(range(n))
    half = n // 2
    near = sorted(range(1, half), key=lambda k: (-k.bit_count(), k))
    return [0, half] + near + [half + k for k in near]


def gather_col(x, n):
    half = n // 2
    parts = {0: x}
    for k in col_order(n)[1:]:
        relayed = n >= 4 and pow2(n) and k > half
        parts[k] = permute(parts[half] if relayed else x, "col", k - half if relayed else k, n)
    return [((k,), part) for k, part in parts.items()]


def gather_col_joined(x, n):
    if n < 4 or not pow2(n):
        return gather_col(x, n)
    half = n // 2
    both = jnp.concatenate([x, permute(x, "col", half, n)])
    parts = [((0, half), both)]
    for k in col_order(n)[2 : 1 + half]:
        parts.append(((k, half + k), permute(both, "col", k, n)))
    return parts


BIG = 1 << 20
STEP = 1 << 10


def wants(target, owner, group, tables, dims):
    xs, xc, ss, sc = tables
    caps, tile_width = dims
    near, far = [], []
    for q in range(group):
        cw = owner * group + q
        for a in range(CAPW):
            p = xs[target, cw, a]
            column = jnp.where(a < xc[target, cw], p % tile_width, -1)
            near.append((q * RB + p // tile_width, column, cw * CAPW + a))
        for v in range(caps):
            p = ss[target, v, cw]
            column = jnp.where(v < sc[target, cw], p % JW, -1)
            far.append((q * RB + p // JW, column, cw * caps + v))
    return near, far


def outputs(target, c, tables, dims):
    xs, xc, ss, sc = tables
    caps, tile_width = dims
    found = []
    for t in range(caps):
        o = ss[target, t, c]
        found.append((o // JW * tile_width, jnp.where(t < sc[target, c], o % JW, -2)))
    return found


def fill(table, xs, xc, rho, c, capacity):
    live = xc[rho, c]
    for s in reversed(range(capacity)):
        table[xs[rho, c, s]] = jnp.where(s < live, s + 1, 0)


def unfill(table, xs, rho, c, capacity):
    for s in range(capacity):
        table[xs[rho, c, s]] = 0


def clear(table, size):
    def one(i, carry):
        table[i] = 0
        return carry

    lax.fori_loop(0, size, one, 0, unroll=16)


def send_kernel(sizes, *refs):
    nr, nc, capacity, caps, limits, tile_width = sizes
    tables, x = refs[:4], refs[4]
    outs = refs[5 : 5 + nr]
    own, table, picks = refs[5 + nr :]
    group, dims = tile_width // RB, (caps, tile_width)
    xs, xc, ss, sc = tables
    r, c = lax.axis_index("row"), lax.axis_index("col")
    clear(table, RB * tile_width)
    fill(table, xs, xc, r, c, capacity)
    for k in range(nr):
        target = origin(r, k if pow2(nr) else (nr - k) % nr, nr)
        near, far = wants(target, r, group, tables, dims)
        total = jnp.int32(0)
        for base, j in outputs(target, c, tables, dims):
            for inner, column, _ in near + far:
                slot = table[base + inner]
                picks[total] = slot - 1
                total = total + ((column == j) & (slot > 0)).astype(jnp.int32)

        def copy(n, carry, k=k):
            outs[k][n] = x[picks[n]]
            return carry

        lax.fori_loop(0, jnp.minimum(total, limits[k]), copy, 0)
    for t, (base, j) in enumerate(outputs(r, c, tables, dims)):
        slot = jnp.where(j >= 0, table[base + jnp.maximum(j, 0)], 0)
        block = x[jnp.maximum(slot - 1, 0)]
        own[t] = jnp.where(slot > 0, block, jnp.zeros_like(block))


def plan_kernel(sizes, whole, *refs):
    nr, nc, capacity, caps, limits, tile_width = sizes
    tables = refs[:4]
    near_ref, far_ref, count, table = refs[4:]
    group, dims = tile_width // RB, (caps, tile_width)
    xs, xc, ss, sc = tables
    r, c = lax.axis_index("row"), lax.axis_index("col")
    clear(table, RB * tile_width)
    mine = outputs(r, c, tables, dims)

    def per_source(e, carry):
        rho = origin(r, e, nr)
        fill(table, xs, xc, rho, c, capacity)
        near, far = wants(r, rho, group, tables, dims)
        total, n_near, n_far = jnp.int32(0), jnp.int32(0), jnp.int32(0)
        for t, (base, j) in enumerate(mine):
            for inner, column, right in near:
                slot = table[base + inner]
                left = jnp.maximum(slot - 1, 0) if whole else total
                near_ref[e, n_near] = left + 64 * t + 256 * right
                hit = ((column == j) & (slot > 0)).astype(jnp.int32)
                n_near, total = n_near + hit, total + hit
            for inner, column, right in far:
                slot = table[base + inner]
                left = jnp.maximum(slot - 1, 0) if whole else total
                far_ref[e, n_far] = left + 64 * t + 256 * right
                hit = ((column == j) & (slot > 0)).astype(jnp.int32)
                n_far, total = n_far + hit, total + hit
        count[e, 0] = n_near
        count[e, 1] = n_far
        unfill(table, xs, rho, c, capacity)
        return carry

    lax.fori_loop(0, nr, per_source, 0)


def count_kernel(sizes, *refs):
    nr, nc, capacity, caps, limits, tile_width = sizes
    tables = refs[:4]
    slots_ref, message, over, square, hits, sent = refs[4:]
    sending = pltpu.make_async_copy(message, square, sent)
    sending.start()
    group, dims = tile_width // RB, (caps, tile_width)
    xs, xc, ss, sc = tables
    rows = lax.broadcasted_iota(jnp.int32, (nc, capacity), 0)
    lanes = lax.broadcasted_iota(jnp.int32, (nc, capacity), 1)

    def loop(n, body):
        if n <= 4:
            for i in range(n):
                body(i)
        else:
            lax.fori_loop(0, n, lambda i, carry: body(i) or carry, 0)

    def column_of(read):
        made = jnp.zeros((nc, capacity), jnp.int32)
        for i in range(nc):
            made = jnp.where(rows == i, read(i), made)
        return made

    held_of = [None] * nr
    for rho in range(nr if nr <= 4 else 0):
        live = lanes < column_of(lambda i: xc[rho, i])
        held_of[rho] = jnp.where(live, slots_ref[rho], -4 * BIG)

    def per_target(target):
        keys = []
        for t in range(caps):

            def key(i):
                o = ss[target, t, i]
                return jnp.where(t < sc[target, i], o // JW * tile_width - o % JW * STEP, BIG)

            keys.append(column_of(key))

        def per_owner(rho):
            if nr <= 4:
                held = held_of[rho]
            else:
                live = lanes < column_of(lambda i: xc[rho, i])
                held = jnp.where(live, slots_ref[rho], -4 * BIG)
            near, far = wants(target, rho, group, tables, dims)
            scalars = [jnp.where(col < 0, -BIG * 8, inn + col * STEP) for inn, col, _ in near + far]
            found = jnp.zeros((nc, capacity), jnp.int32)
            for key in keys:
                apart = held - key
                for scalar in scalars:
                    found = found + (apart == scalar).astype(jnp.int32)
            spare = jnp.where(rho == target, limits[0], limits[1])
            hits[target * nr + rho] = jnp.where(lanes == 0, found - spare, found)

        loop(nr, per_owner)

    lax.fori_loop(0, nr, lambda i, carry: per_target(i) or carry, 0)
    longest = jnp.max(jnp.sum(hits[...], axis=2))
    over[0] = (longest > 0).astype(jnp.int32)
    sending.wait()


def product_kernel(sizes, final, *refs):
    nr, nc, per, limits, offsets = sizes
    codes, count = refs[:2]
    rights = refs[2 : 2 + len(offsets)]
    lefts = refs[2 + len(offsets) : 2 + len(offsets) + nr]
    rest = refs[2 + len(offsets) + nr :]
    held, total = rest[-2:]
    c = lax.axis_index("col")
    for ks, right in zip(offsets, rights):
        for i, k in enumerate(ks):
            held[pl.ds(origin(c, k, nc) * per, per)] = right[i * per : (i + 1) * per]
    total[...] = jnp.zeros_like(total)
    for e in range(nr):

        def step(n, carry, e=e):
            code = codes[e, n]
            left = lefts[e][jnp.minimum(code % 64, limits[e] - 1)]
            right = held[code // 256]
            t = code // 64 % 4
            total[t] += jnp.dot(left, right, preferred_element_type=jnp.float32)
            return carry

        lax.fori_loop(0, count[e, 1 if final else 0], step, 0)
    if final:
        own, out = rest[:2]
        out[...] = (1.5 * own[...].astype(jnp.float32) - 0.5 * total[...]).astype(out.dtype)
    else:
        rest[0][...] = total[...].astype(rest[0].dtype)


def smem():
    return pl.BlockSpec(memory_space=pltpu.SMEM)


def vmem():
    return pl.BlockSpec(memory_space=pltpu.VMEM)


def grant(blocks):
    return pltpu.CompilerParams(vmem_limit_bytes=(blocks + 64) * 32768)


def plan(sizes, whole, tables):
    nr, nc, capacity, caps, limits, tile_width = sizes
    group = tile_width // RB
    shapes = [(nr, caps * group * CAPW + 1), (nr, caps * group * caps + 1), (nr, 2)]
    return pl.pallas_call(
        lambda *refs: plan_kernel(sizes, whole, *refs),
        out_shape=[jax.ShapeDtypeStruct(shape, jnp.int32) for shape in shapes],
        in_specs=[smem()] * 4,
        out_specs=[smem()] * 3,
        scratch_shapes=[pltpu.SMEM((RB * tile_width,), jnp.int32)],
        compiler_params=grant(0),
        name="plan",
    )(*tables)


def product(sizes, caps, per, codes, count, gathered, lefts, own=None):
    nr, nc = sizes
    size = lefts[0].shape[1]
    offsets, rights = zip(*gathered)
    limits = [left.shape[0] for left in lefts]
    extra = [] if own is None else [own]
    return pl.pallas_call(
        lambda *refs: product_kernel((nr, nc, per, limits, offsets), own is not None, *refs),
        out_shape=jax.ShapeDtypeStruct((caps, size, size), jnp.bfloat16),
        in_specs=[smem()] * 2 + [vmem()] * (nr + len(rights) + len(extra)),
        out_specs=vmem(),
        scratch_shapes=[
            pltpu.VMEM((nc * per, size, size), jnp.bfloat16),
            pltpu.VMEM((caps, size, size), jnp.float32),
        ],
        compiler_params=grant(sum(limits) + 2 * nc * per + 6 * caps),
        name="first" if own is None else "second",
    )(codes, count, *rights, *lefts, *extra)


def general(tile, tables, windows, own, sizes):
    nr, nc, caps = sizes[0], sizes[1], sizes[3]
    near, far, count = plan(sizes, True, tables)
    lefts = [tile] + [permute(tile, "row", k, nr) for k in range(1, nr)]
    square = product((nr, nc), caps, CAPW, near, count, windows, lefts)
    everything = gather_col(square, nc)
    return square, product((nr, nc), caps, caps, far, count, everything, lefts, own)


def local(x_blocks, x_slots, x_count, s_slots, s_count):
    nr, nc = lax.axis_size("row"), lax.axis_size("col")
    capacity, size = x_blocks.shape[2], x_blocks.shape[3]
    caps = s_slots.shape[2]
    tile_width = RB * nc // nr
    group = tile_width // RB
    assert nc % nr == 0 and caps <= 4 and capacity <= 64
    tile = x_blocks.reshape(capacity, size, size)
    block = jax.ShapeDtypeStruct
    limits = [min(capacity, 4 * group)] + [min(capacity, 5 * group // 2)] * (nr - 1)
    sizes = (nr, nc, capacity, caps, limits, tile_width)
    tables = (x_slots, x_count, s_slots.transpose(0, 2, 1), s_count)
    made = pl.pallas_call(
        lambda *refs: send_kernel(sizes, *refs),
        out_shape=[block((n, size, size), tile.dtype) for n in limits]
        + [block((caps, size, size), tile.dtype)],
        in_specs=[smem()] * 4 + [vmem()],
        out_specs=[vmem()] * (nr + 1),
        scratch_shapes=[
            pltpu.SMEM((RB * tile_width,), jnp.int32),
            pltpu.SMEM((caps * group * (CAPW + caps) + 1,), jnp.int32),
        ],
        compiler_params=grant(capacity + sum(limits) + caps),
        name="send",
    )(*tables, tile)
    sends, own = made[:nr], made[nr]
    near, far, count = plan(sizes, False, tables)
    windows = gather_col_joined(tile[:CAPW], nc)
    lefts = [sends[0]] + [permute(sends[k], "row", k, nr) for k in range(1, nr)]
    message = product((nr, nc), caps, CAPW, near, count, windows, lefts)
    over, square = pl.pallas_call(
        lambda *refs: count_kernel(sizes, *refs),
        out_shape=[block((1,), jnp.int32), block(message.shape, message.dtype)],
        in_specs=[smem()] * 4 + [vmem()] * 2,
        out_specs=[smem(), pl.BlockSpec(memory_space=pltpu.HBM)],
        scratch_shapes=[pltpu.VMEM((nr * nr, nc, capacity), jnp.int32), pltpu.SemaphoreType.DMA],
        compiler_params=grant(2 * caps),
        name="count",
    )(*tables, x_slots, message)
    everything = gather_col(message, nc)
    result = product((nr, nc), caps, caps, far, count, everything, lefts, own)
    offsets, windows = zip(*windows)
    square, result = lax.cond(
        over[0] > 0,
        lambda t, w, o, s, u, *tables: general(t, tables, list(zip(offsets, w)), o, sizes),
        lambda t, w, o, s, u, *tables: (s, u),
        *(tile, windows, own, square, result, *tables),
    )
    return square[None, None], result[None, None]


def solution(mesh):
    spec = P("row", "col", None, None, None)
    return jax.shard_map(
        local,
        mesh=mesh,
        in_specs=(spec, P(), P(), P(), P()),
        out_specs=(spec, spec),
        check_vma=False,
    )
```

```python
import jax
import jax.numpy as jnp
from jax import lax
from jax.experimental import pallas as pl
from jax.experimental.pallas import tpu as pltpu
from jax.sharding import PartitionSpec as P

RB = 8
JW = 2
CAPW = 2


def pow2(n):
    return n & (n - 1) == 0


def partner(i, k, n):
    return i ^ k if pow2(n) else (i + k) % n


def origin(i, k, n):
    return jnp.bitwise_xor(i, k) if pow2(n) else lax.rem(i + (n - k), n)


def permute(x, axis, k, n):
    return lax.ppermute(x, axis, [(i, partner(i, k, n)) for i in range(n)])


def col_order(n):
    if n < 4 or not pow2(n):
        return list(range(n))
    half = n // 2
    near = sorted(range(1, half), key=lambda k: (-k.bit_count(), k))
    return [0, half] + near + [half + k for k in near]


def gather_col(x, n):
    half = n // 2
    parts = {0: x}
    for k in col_order(n)[1:]:
        relayed = n >= 4 and pow2(n) and k > half
        parts[k] = permute(parts[half] if relayed else x, "col", k - half if relayed else k, n)
    return [((k,), part) for k, part in parts.items()]


def gather_col_joined(x, n):
    if n < 4 or not pow2(n):
        return gather_col(x, n)
    half = n // 2
    both = jnp.concatenate([x, permute(x, "col", half, n)])
    parts = [((0, half), both)]
    for k in col_order(n)[2 : 1 + half]:
        parts.append(((k, half + k), permute(both, "col", k, n)))
    return parts


BIG = 1 << 20
STEP = 1 << 10


def wants(target, owner, group, tables, dims):
    xs, xc, ss, sc = tables
    caps, tile_width = dims
    near, far = [], []
    for q in range(group):
        cw = owner * group + q
        for a in range(CAPW):
            p = xs[target, cw, a]
            column = jnp.where(a < xc[target, cw], p % tile_width, -1)
            near.append((q * RB + p // tile_width, column, cw * CAPW + a))
        for v in range(caps):
            p = ss[target, v, cw]
            column = jnp.where(v < sc[target, cw], p % JW, -1)
            far.append((q * RB + p // JW, column, cw * caps + v))
    return near, far


def outputs(target, c, tables, dims):
    xs, xc, ss, sc = tables
    caps, tile_width = dims
    found = []
    for t in range(caps):
        o = ss[target, t, c]
        found.append((o // JW * tile_width, jnp.where(t < sc[target, c], o % JW, -2)))
    return found


def fill(table, xs, xc, rho, c, capacity):
    live = xc[rho, c]
    for s in reversed(range(capacity)):
        table[xs[rho, c, s]] = jnp.where(s < live, s + 1, 0)


def unfill(table, xs, rho, c, capacity):
    for s in range(capacity):
        table[xs[rho, c, s]] = 0


def clear(table, size):
    def one(i, carry):
        table[i] = 0
        return carry

    lax.fori_loop(0, size, one, 0, unroll=16)


def send_kernel(sizes, *refs):
    nr, nc, capacity, caps, limits, tile_width = sizes
    tables, x = refs[:4], refs[4]
    outs = refs[5 : 5 + nr]
    own, table, picks = refs[5 + nr :]
    group, dims = tile_width // RB, (caps, tile_width)
    xs, xc, ss, sc = tables
    r, c = lax.axis_index("row"), lax.axis_index("col")
    clear(table, RB * tile_width)
    fill(table, xs, xc, r, c, capacity)
    for k in range(nr):
        target = origin(r, k if pow2(nr) else (nr - k) % nr, nr)
        near, far = wants(target, r, group, tables, dims)
        total = jnp.int32(0)
        for base, j in outputs(target, c, tables, dims):
            for inner, column, _ in near + far:
                slot = table[base + inner]
                picks[total] = slot - 1
                total = total + ((column == j) & (slot > 0)).astype(jnp.int32)

        def copy(n, carry, k=k):
            outs[k][n] = x[picks[n]]
            return carry

        lax.fori_loop(0, jnp.minimum(total, limits[k]), copy, 0)
    for t, (base, j) in enumerate(outputs(r, c, tables, dims)):
        slot = jnp.where(j >= 0, table[base + jnp.maximum(j, 0)], 0)
        block = x[jnp.maximum(slot - 1, 0)]
        own[t] = jnp.where(slot > 0, block, jnp.zeros_like(block))


def plan_kernel(sizes, whole, *refs):
    nr, nc, capacity, caps, limits, tile_width = sizes
    tables = refs[:4]
    near_ref, far_ref, count, table = refs[4:]
    group, dims = tile_width // RB, (caps, tile_width)
    xs, xc, ss, sc = tables
    r, c = lax.axis_index("row"), lax.axis_index("col")
    clear(table, RB * tile_width)
    mine = outputs(r, c, tables, dims)

    def per_source(e, carry):
        rho = origin(r, e, nr)
        fill(table, xs, xc, rho, c, capacity)
        near, far = wants(r, rho, group, tables, dims)
        total, n_near, n_far = jnp.int32(0), jnp.int32(0), jnp.int32(0)
        for t, (base, j) in enumerate(mine):
            for inner, column, right in near:
                slot = table[base + inner]
                left = jnp.maximum(slot - 1, 0) if whole else total
                near_ref[e, n_near] = left + 64 * t + 256 * right
                hit = ((column == j) & (slot > 0)).astype(jnp.int32)
                n_near, total = n_near + hit, total + hit
            for inner, column, right in far:
                slot = table[base + inner]
                left = jnp.maximum(slot - 1, 0) if whole else total
                far_ref[e, n_far] = left + 64 * t + 256 * right
                hit = ((column == j) & (slot > 0)).astype(jnp.int32)
                n_far, total = n_far + hit, total + hit
        count[e, 0] = n_near
        count[e, 1] = n_far
        unfill(table, xs, rho, c, capacity)
        return carry

    lax.fori_loop(0, nr, per_source, 0)


def count_kernel(sizes, *refs):
    nr, nc, capacity, caps, limits, tile_width = sizes
    tables = refs[:4]
    slots_ref, message, over, square, hits, sent = refs[4:]
    sending = pltpu.make_async_copy(message, square, sent)
    sending.start()
    group, dims = tile_width // RB, (caps, tile_width)
    xs, xc, ss, sc = tables
    rows = lax.broadcasted_iota(jnp.int32, (nc, capacity), 0)
    lanes = lax.broadcasted_iota(jnp.int32, (nc, capacity), 1)

    def loop(n, body):
        if n <= 4:
            for i in range(n):
                body(i)
        else:
            lax.fori_loop(0, n, lambda i, carry: body(i) or carry, 0)

    def column_of(read):
        made = jnp.zeros((nc, capacity), jnp.int32)
        for i in range(nc):
            made = jnp.where(rows == i, read(i), made)
        return made

    held_of = [None] * nr
    for rho in range(nr if nr <= 4 else 0):
        live = lanes < column_of(lambda i: xc[rho, i])
        held_of[rho] = jnp.where(live, slots_ref[rho], -4 * BIG)

    def per_target(target):
        keys = []
        for t in range(caps):

            def key(i):
                o = ss[target, t, i]
                return jnp.where(t < sc[target, i], o // JW * tile_width - o % JW * STEP, BIG)

            keys.append(column_of(key))

        def per_owner(rho):
            if nr <= 4:
                held = held_of[rho]
            else:
                live = lanes < column_of(lambda i: xc[rho, i])
                held = jnp.where(live, slots_ref[rho], -4 * BIG)
            near, far = wants(target, rho, group, tables, dims)
            scalars = [jnp.where(col < 0, -BIG * 8, inn + col * STEP) for inn, col, _ in near + far]
            found = jnp.zeros((nc, capacity), jnp.int32)
            for key in keys:
                apart = held - key
                for scalar in scalars:
                    found = found + (apart == scalar).astype(jnp.int32)
            spare = jnp.where(rho == target, limits[0], limits[1])
            hits[target * nr + rho] = jnp.where(lanes == 0, found - spare, found)

        loop(nr, per_owner)

    lax.fori_loop(0, nr, lambda i, carry: per_target(i) or carry, 0)
    longest = jnp.max(jnp.sum(hits[...], axis=2))
    over[0] = (longest > 0).astype(jnp.int32)
    sending.wait()


def product_kernel(sizes, final, *refs):
    nr, nc, per, limits, offsets = sizes
    codes, count = refs[:2]
    rights = refs[2 : 2 + len(offsets)]
    lefts = refs[2 + len(offsets) : 2 + len(offsets) + nr]
    lefts = lefts[:1] + lefts[:0:-1]
    rest = refs[2 + len(offsets) + nr :]
    held, total = rest[-2:]
    c = lax.axis_index("col")
    for ks, right in zip(offsets, rights):
        for i, k in enumerate(ks):
            held[pl.ds(origin(c, k, nc) * per, per)] = right[i * per : (i + 1) * per]
    total[...] = jnp.zeros_like(total)
    for e in range(nr):

        def step(n, carry, e=e):
            code = codes[e, n]
            left = lefts[e][jnp.minimum(code % 64, limits[e] - 1)]
            right = held[code // 256]
            t = code // 64 % 4
            total[t] += jnp.dot(left, right, preferred_element_type=jnp.float32)
            return carry

        lax.fori_loop(0, count[e, 1 if final else 0], step, 0)
    if final:
        own, out = rest[:2]
        out[...] = (1.5 * own[...].astype(jnp.float32) - 0.5 * total[...]).astype(out.dtype)
    else:
        rest[0][...] = total[...].astype(rest[0].dtype)


def smem():
    return pl.BlockSpec(memory_space=pltpu.SMEM)


def vmem():
    return pl.BlockSpec(memory_space=pltpu.VMEM)


def grant(blocks):
    return pltpu.CompilerParams(vmem_limit_bytes=(blocks + 64) * 32768)


def plan(sizes, whole, tables):
    nr, nc, capacity, caps, limits, tile_width = sizes
    group = tile_width // RB
    shapes = [(nr, caps * group * CAPW + 1), (nr, caps * group * caps + 1), (nr, 2)]
    return pl.pallas_call(
        lambda *refs: plan_kernel(sizes, whole, *refs),
        out_shape=[jax.ShapeDtypeStruct(shape, jnp.int32) for shape in shapes],
        in_specs=[smem()] * 4,
        out_specs=[smem()] * 3,
        scratch_shapes=[pltpu.SMEM((RB * tile_width,), jnp.int32)],
        compiler_params=grant(0),
        name="plan",
    )(*tables)


def product(sizes, caps, per, codes, count, gathered, lefts, own=None):
    nr, nc = sizes
    size = lefts[0].shape[1]
    offsets, rights = zip(*gathered)
    limits = [left.shape[0] for left in lefts]
    extra = [] if own is None else [own]
    return pl.pallas_call(
        lambda *refs: product_kernel((nr, nc, per, limits, offsets), own is not None, *refs),
        out_shape=jax.ShapeDtypeStruct((caps, size, size), jnp.bfloat16),
        in_specs=[smem()] * 2 + [vmem()] * (nr + len(rights) + len(extra)),
        out_specs=vmem(),
        scratch_shapes=[
            pltpu.VMEM((nc * per, size, size), jnp.bfloat16),
            pltpu.VMEM((caps, size, size), jnp.float32),
        ],
        compiler_params=grant(sum(limits) + 2 * nc * per + 6 * caps),
        name="first" if own is None else "second",
    )(codes, count, *rights, *lefts[:1], *lefts[:0:-1], *extra)


def general(tile, tables, windows, own, sizes):
    nr, nc, caps = sizes[0], sizes[1], sizes[3]
    near, far, count = plan(sizes, True, tables)
    lefts = [tile] + [permute(tile, "row", k, nr) for k in range(1, nr)]
    square = product((nr, nc), caps, CAPW, near, count, windows, lefts)
    everything = gather_col(square, nc)
    return square, product((nr, nc), caps, caps, far, count, everything, lefts, own)


def local(x_blocks, x_slots, x_count, s_slots, s_count):
    nr, nc = lax.axis_size("row"), lax.axis_size("col")
    capacity, size = x_blocks.shape[2], x_blocks.shape[3]
    caps = s_slots.shape[2]
    tile_width = RB * nc // nr
    group = tile_width // RB
    assert nc % nr == 0 and caps <= 4 and capacity <= 64
    tile = x_blocks.reshape(capacity, size, size)
    block = jax.ShapeDtypeStruct
    limits = [min(capacity, 4 * group)] + [min(capacity, 5 * group // 2)] * (nr - 1)
    sizes = (nr, nc, capacity, caps, limits, tile_width)
    tables = (x_slots, x_count, s_slots.transpose(0, 2, 1), s_count)
    made = pl.pallas_call(
        lambda *refs: send_kernel(sizes, *refs),
        out_shape=[block((n, size, size), tile.dtype) for n in limits]
        + [block((caps, size, size), tile.dtype)],
        in_specs=[smem()] * 4 + [vmem()],
        out_specs=[vmem()] * (nr + 1),
        scratch_shapes=[
            pltpu.SMEM((RB * tile_width,), jnp.int32),
            pltpu.SMEM((caps * group * (CAPW + caps) + 1,), jnp.int32),
        ],
        compiler_params=grant(capacity + sum(limits) + caps),
        name="send",
    )(*tables, tile)
    sends, own = made[:nr], made[nr]
    near, far, count = plan(sizes, False, tables)
    windows = gather_col_joined(tile[:CAPW], nc)
    lefts = [sends[0]] + [permute(sends[k], "row", k, nr) for k in range(1, nr)]
    message = product((nr, nc), caps, CAPW, near, count, windows, lefts)
    over, square = pl.pallas_call(
        lambda *refs: count_kernel(sizes, *refs),
        out_shape=[block((1,), jnp.int32), block(message.shape, message.dtype)],
        in_specs=[smem()] * 4 + [vmem()] * 2,
        out_specs=[smem(), pl.BlockSpec(memory_space=pltpu.HBM)],
        scratch_shapes=[pltpu.VMEM((nr * nr, nc, capacity), jnp.int32), pltpu.SemaphoreType.DMA],
        compiler_params=grant(2 * caps),
        name="count",
    )(*tables, x_slots, message)
    everything = gather_col(message, nc)
    result = product((nr, nc), caps, caps, far, count, everything, lefts, own)
    offsets, windows = zip(*windows)
    square, result = lax.cond(
        over[0] > 0,
        lambda t, w, o, s, u, *tables: general(t, tables, list(zip(offsets, w)), o, sizes),
        lambda t, w, o, s, u, *tables: (s, u),
        *(tile, windows, own, square, result, *tables),
    )
    return square[None, None], result[None, None]


def solution(mesh):
    spec = P("row", "col", None, None, None)
    return jax.shard_map(
        local,
        mesh=mesh,
        in_specs=(spec, P(), P(), P(), P()),
        out_specs=(spec, spec),
        check_vma=False,
    )
```

```python
import jax
import jax.numpy as jnp
from jax import lax
from jax.experimental import pallas as pl
from jax.experimental.pallas import tpu as pltpu
from jax.sharding import PartitionSpec as P

RB = 8
JW = 2
CAPW = 2


def pow2(n):
    return n & (n - 1) == 0


def partner(i, k, n):
    return i ^ k if pow2(n) else (i + k) % n


def origin(i, k, n):
    return jnp.bitwise_xor(i, k) if pow2(n) else lax.rem(i + (n - k), n)


def permute(x, axis, k, n):
    return lax.ppermute(x, axis, [(i, partner(i, k, n)) for i in range(n)])


def crossed(k, odd):
    low = k & 3
    return k ^ 3 if odd and low in (1, 2) else k


def permute_col(x, k, nr, nc):
    if not pow2(nc) or nr % 2:
        return permute(x, "col", k, nc)
    pairs = [
        (r * nc + c, r * nc + (c ^ crossed(k, r % 2))) for r in range(nr) for c in range(nc)
    ]
    return lax.ppermute(x, ("row", "col"), pairs)


def source_col(c, k, nr, nc):
    if not pow2(nc) or nr % 2:
        return origin(c, k, nc)
    odd = lax.rem(lax.axis_index("row"), 2) > 0
    return jnp.bitwise_xor(c, jnp.where(odd, crossed(k, 1), k))


def col_order(n):
    if n < 4 or not pow2(n):
        return list(range(n))
    half = n // 2
    near = sorted(range(1, half), key=lambda k: (k.bit_count(), k))
    return [0, half] + near + [half + k for k in near]


def gather_col(x, n, nr):
    half = n // 2
    parts = {0: x}
    for k in col_order(n)[1:]:
        relayed = n >= 4 and pow2(n) and k > half
        parts[k] = permute_col(parts[half] if relayed else x, k - half if relayed else k, nr, n)
    return [((k,), part) for k, part in parts.items()]


def gather_col_joined(x, n, nr):
    if n < 4 or not pow2(n):
        return gather_col(x, n, nr)
    half = n // 2
    both = jnp.concatenate([x, permute_col(x, half, nr, n)])
    parts = [((0, half), both)]
    for k in col_order(n)[2 : 1 + half]:
        parts.append(((k, half + k), permute_col(both, k, nr, n)))
    return parts


BIG = 1 << 20
STEP = 1 << 10


def wants(target, owner, group, tables, dims):
    xs, xc, ss, sc = tables
    caps, tile_width = dims
    near, far = [], []
    for q in range(group):
        cw = owner * group + q
        for a in range(CAPW):
            p = xs[target, cw, a]
            column = jnp.where(a < xc[target, cw], p % tile_width, -1)
            near.append((q * RB + p // tile_width, column, cw * CAPW + a))
        for v in range(caps):
            p = ss[target, v, cw]
            column = jnp.where(v < sc[target, cw], p % JW, -1)
            far.append((q * RB + p // JW, column, cw * caps + v))
    return near, far


def outputs(target, c, tables, dims):
    xs, xc, ss, sc = tables
    caps, tile_width = dims
    found = []
    for t in range(caps):
        o = ss[target, t, c]
        found.append((o // JW * tile_width, jnp.where(t < sc[target, c], o % JW, -2)))
    return found


def fill(table, xs, xc, rho, c, capacity):
    live = xc[rho, c]
    for s in reversed(range(capacity)):
        table[xs[rho, c, s]] = jnp.where(s < live, s + 1, 0)


def unfill(table, xs, rho, c, capacity):
    for s in range(capacity):
        table[xs[rho, c, s]] = 0


def clear(table, size):
    def one(i, carry):
        table[i] = 0
        return carry

    lax.fori_loop(0, size, one, 0, unroll=16)


def send_kernel(sizes, *refs):
    nr, nc, capacity, caps, limits, tile_width = sizes
    tables, x = refs[:4], refs[4]
    outs = refs[5 : 5 + nr]
    own, table, picks = refs[5 + nr :]
    group, dims = tile_width // RB, (caps, tile_width)
    xs, xc, ss, sc = tables
    r, c = lax.axis_index("row"), lax.axis_index("col")
    clear(table, RB * tile_width)
    fill(table, xs, xc, r, c, capacity)
    for k in range(nr):
        target = origin(r, k if pow2(nr) else (nr - k) % nr, nr)
        near, far = wants(target, r, group, tables, dims)
        total = jnp.int32(0)
        for base, j in outputs(target, c, tables, dims):
            for inner, column, _ in near + far:
                slot = table[base + inner]
                picks[total] = slot - 1
                total = total + ((column == j) & (slot > 0)).astype(jnp.int32)

        def copy(n, carry, k=k):
            outs[k][n] = x[picks[n]]
            return carry

        lax.fori_loop(0, jnp.minimum(total, limits[k]), copy, 0)
    for t, (base, j) in enumerate(outputs(r, c, tables, dims)):
        slot = jnp.where(j >= 0, table[base + jnp.maximum(j, 0)], 0)
        block = x[jnp.maximum(slot - 1, 0)]
        own[t] = jnp.where(slot > 0, block, jnp.zeros_like(block))


def plan_kernel(sizes, whole, *refs):
    nr, nc, capacity, caps, limits, tile_width = sizes
    tables = refs[:4]
    near_ref, far_ref, count, table = refs[4:]
    group, dims = tile_width // RB, (caps, tile_width)
    xs, xc, ss, sc = tables
    r, c = lax.axis_index("row"), lax.axis_index("col")
    clear(table, RB * tile_width)
    mine = outputs(r, c, tables, dims)

    def per_source(e, carry):
        rho = origin(r, e, nr)
        fill(table, xs, xc, rho, c, capacity)
        near, far = wants(r, rho, group, tables, dims)
        total, n_near, n_far = jnp.int32(0), jnp.int32(0), jnp.int32(0)
        for t, (base, j) in enumerate(mine):
            for inner, column, right in near:
                slot = table[base + inner]
                left = jnp.maximum(slot - 1, 0) if whole else total
                near_ref[e, n_near] = left + 64 * t + 256 * right
                hit = ((column == j) & (slot > 0)).astype(jnp.int32)
                n_near, total = n_near + hit, total + hit
            for inner, column, right in far:
                slot = table[base + inner]
                left = jnp.maximum(slot - 1, 0) if whole else total
                far_ref[e, n_far] = left + 64 * t + 256 * right
                hit = ((column == j) & (slot > 0)).astype(jnp.int32)
                n_far, total = n_far + hit, total + hit
        count[e, 0] = n_near
        count[e, 1] = n_far
        unfill(table, xs, rho, c, capacity)
        return carry

    lax.fori_loop(0, nr, per_source, 0)


def count_kernel(sizes, *refs):
    nr, nc, capacity, caps, limits, tile_width = sizes
    tables = refs[:4]
    slots_ref, message, over, square, hits, sent = refs[4:]
    sending = pltpu.make_async_copy(message, square, sent)
    sending.start()
    group, dims = tile_width // RB, (caps, tile_width)
    xs, xc, ss, sc = tables
    rows = lax.broadcasted_iota(jnp.int32, (nc, capacity), 0)
    lanes = lax.broadcasted_iota(jnp.int32, (nc, capacity), 1)

    def loop(n, body):
        if n <= 4:
            for i in range(n):
                body(i)
        else:
            lax.fori_loop(0, n, lambda i, carry: body(i) or carry, 0)

    def column_of(read):
        made = jnp.zeros((nc, capacity), jnp.int32)
        for i in range(nc):
            made = jnp.where(rows == i, read(i), made)
        return made

    held_of = [None] * nr
    for rho in range(nr if nr <= 4 else 0):
        live = lanes < column_of(lambda i: xc[rho, i])
        held_of[rho] = jnp.where(live, slots_ref[rho], -4 * BIG)

    def per_target(target):
        keys = []
        for t in range(caps):

            def key(i):
                o = ss[target, t, i]
                return jnp.where(t < sc[target, i], o // JW * tile_width - o % JW * STEP, BIG)

            keys.append(column_of(key))

        def per_owner(rho):
            if nr <= 4:
                held = held_of[rho]
            else:
                live = lanes < column_of(lambda i: xc[rho, i])
                held = jnp.where(live, slots_ref[rho], -4 * BIG)
            near, far = wants(target, rho, group, tables, dims)
            scalars = [jnp.where(col < 0, -BIG * 8, inn + col * STEP) for inn, col, _ in near + far]
            found = jnp.zeros((nc, capacity), jnp.int32)
            for key in keys:
                apart = held - key
                for scalar in scalars:
                    found = found + (apart == scalar).astype(jnp.int32)
            spare = jnp.where(rho == target, limits[0], limits[1])
            hits[target * nr + rho] = jnp.where(lanes == 0, found - spare, found)

        loop(nr, per_owner)

    lax.fori_loop(0, nr, lambda i, carry: per_target(i) or carry, 0)
    longest = jnp.max(jnp.sum(hits[...], axis=2))
    over[0] = (longest > 0).astype(jnp.int32)
    sending.wait()


def product_kernel(sizes, final, *refs):
    nr, nc, per, limits, offsets = sizes
    codes, count = refs[:2]
    rights = refs[2 : 2 + len(offsets)]
    lefts = refs[2 + len(offsets) : 2 + len(offsets) + nr]
    rest = refs[2 + len(offsets) + nr :]
    held, total = rest[-2:]
    c = lax.axis_index("col")
    for ks, right in zip(offsets, rights):
        for i, k in enumerate(ks):
            held[pl.ds(source_col(c, k, nr, nc) * per, per)] = right[i * per : (i + 1) * per]
    total[...] = jnp.zeros_like(total)
    for e in range(nr):

        def step(n, carry, e=e):
            code = codes[e, n]
            left = lefts[e][jnp.minimum(code % 64, limits[e] - 1)]
            right = held[code // 256]
            t = code // 64 % 4
            total[t] += jnp.dot(left, right, preferred_element_type=jnp.float32)
            return carry

        lax.fori_loop(0, count[e, 1 if final else 0], step, 0)
    if final:
        own, out = rest[:2]
        out[...] = (1.5 * own[...].astype(jnp.float32) - 0.5 * total[...]).astype(out.dtype)
    else:
        rest[0][...] = total[...].astype(rest[0].dtype)


def smem():
    return pl.BlockSpec(memory_space=pltpu.SMEM)


def vmem():
    return pl.BlockSpec(memory_space=pltpu.VMEM)


def grant(blocks):
    return pltpu.CompilerParams(vmem_limit_bytes=(blocks + 64) * 32768)


def plan(sizes, whole, tables):
    nr, nc, capacity, caps, limits, tile_width = sizes
    group = tile_width // RB
    shapes = [(nr, caps * group * CAPW + 1), (nr, caps * group * caps + 1), (nr, 2)]
    return pl.pallas_call(
        lambda *refs: plan_kernel(sizes, whole, *refs),
        out_shape=[jax.ShapeDtypeStruct(shape, jnp.int32) for shape in shapes],
        in_specs=[smem()] * 4,
        out_specs=[smem()] * 3,
        scratch_shapes=[pltpu.SMEM((RB * tile_width,), jnp.int32)],
        compiler_params=grant(0),
        name="plan",
    )(*tables)


def product(sizes, caps, per, codes, count, gathered, lefts, own=None):
    nr, nc = sizes
    size = lefts[0].shape[1]
    offsets, rights = zip(*gathered)
    limits = [left.shape[0] for left in lefts]
    extra = [] if own is None else [own]
    return pl.pallas_call(
        lambda *refs: product_kernel((nr, nc, per, limits, offsets), own is not None, *refs),
        out_shape=jax.ShapeDtypeStruct((caps, size, size), jnp.bfloat16),
        in_specs=[smem()] * 2 + [vmem()] * (nr + len(rights) + len(extra)),
        out_specs=vmem(),
        scratch_shapes=[
            pltpu.VMEM((nc * per, size, size), jnp.bfloat16),
            pltpu.VMEM((caps, size, size), jnp.float32),
        ],
        compiler_params=grant(sum(limits) + 2 * nc * per + 6 * caps),
        name="first" if own is None else "second",
    )(codes, count, *rights, *lefts, *extra)


def general(tile, tables, windows, own, sizes):
    nr, nc, caps = sizes[0], sizes[1], sizes[3]
    near, far, count = plan(sizes, True, tables)
    lefts = [tile] + [permute(tile, "row", k, nr) for k in range(1, nr)]
    square = product((nr, nc), caps, CAPW, near, count, windows, lefts)
    everything = gather_col(square, nc, nr)
    return square, product((nr, nc), caps, caps, far, count, everything, lefts, own)


def local(x_blocks, x_slots, x_count, s_slots, s_count):
    nr, nc = lax.axis_size("row"), lax.axis_size("col")
    capacity, size = x_blocks.shape[2], x_blocks.shape[3]
    caps = s_slots.shape[2]
    tile_width = RB * nc // nr
    group = tile_width // RB
    assert nc % nr == 0 and caps <= 4 and capacity <= 64
    tile = x_blocks.reshape(capacity, size, size)
    block = jax.ShapeDtypeStruct
    limits = [min(capacity, 4 * group)] + [min(capacity, 5 * group // 2)] * (nr - 1)
    sizes = (nr, nc, capacity, caps, limits, tile_width)
    tables = (x_slots, x_count, s_slots.transpose(0, 2, 1), s_count)
    made = pl.pallas_call(
        lambda *refs: send_kernel(sizes, *refs),
        out_shape=[block((n, size, size), tile.dtype) for n in limits]
        + [block((caps, size, size), tile.dtype)],
        in_specs=[smem()] * 4 + [vmem()],
        out_specs=[vmem()] * (nr + 1),
        scratch_shapes=[
            pltpu.SMEM((RB * tile_width,), jnp.int32),
            pltpu.SMEM((caps * group * (CAPW + caps) + 1,), jnp.int32),
        ],
        compiler_params=grant(capacity + sum(limits) + caps),
        name="send",
    )(*tables, tile)
    sends, own = made[:nr], made[nr]
    near, far, count = plan(sizes, False, tables)
    windows = gather_col_joined(tile[:CAPW], nc, nr)
    lefts = [sends[0]] + [permute(sends[k], "row", k, nr) for k in range(1, nr)]
    message = product((nr, nc), caps, CAPW, near, count, windows, lefts)
    over, square = pl.pallas_call(
        lambda *refs: count_kernel(sizes, *refs),
        out_shape=[block((1,), jnp.int32), block(message.shape, message.dtype)],
        in_specs=[smem()] * 4 + [vmem()] * 2,
        out_specs=[smem(), pl.BlockSpec(memory_space=pltpu.HBM)],
        scratch_shapes=[pltpu.VMEM((nr * nr, nc, capacity), jnp.int32), pltpu.SemaphoreType.DMA],
        compiler_params=grant(2 * caps),
        name="count",
    )(*tables, x_slots, message)
    everything = gather_col(message, nc, nr)
    result = product((nr, nc), caps, caps, far, count, everything, lefts, own)
    offsets, windows = zip(*windows)
    square, result = lax.cond(
        over[0] > 0,
        lambda t, w, o, s, u, *tables: general(t, tables, list(zip(offsets, w)), o, sizes),
        lambda t, w, o, s, u, *tables: (s, u),
        *(tile, windows, own, square, result, *tables),
    )
    return square[None, None], result[None, None]


def solution(mesh):
    spec = P("row", "col", None, None, None)
    return jax.shard_map(
        local,
        mesh=mesh,
        in_specs=(spec, P(), P(), P(), P()),
        out_specs=(spec, spec),
        check_vma=False,
    )
```
